32 devices in a mesh: section: 4 (over z), dp: 2 (over y), mp: 4 (over x, core).
Axes of the slice: x: 2, y: 2, z: 4, core: 2. Of those that a mesh axis runs over, the one named last changes fastest.
Arguments:
- text: bfloat16 [4, 1024, 4096], P('section', ('dp', 'mp')), may hold values from -6 to 6
- patches: bfloat16 [4096, 1024], P(('section', 'dp')), may hold values from -6 to 6
- segments: int32 [4, 2, 512], P('section', 'dp'), may hold values from 0 to 3, never falling along the last dimension, each value on 1 to 256 neighbouring positions
- loss_mask: int32 [4, 1024], P('section', ('dp', 'mp')), may hold values from 0 to 1, as said below
- tile_batch: int32 [2, 8], P('dp'), may hold values from 0 to 3, as said below
- tile_offset: int32 [2, 8], P('dp'), may hold values from 0 to 448, as said below
- attn_gain: float32 [4, 4096], P('section'), may hold values from 0.5 to 2
- w_query: bfloat16 [4, 4096, 2048], P('section', None, 'mp'), may hold values from -0.09375 to 0.09375
- w_kv: bfloat16 [4, 2, 4096, 512], P('section', None, None, 'mp'), may hold values from -0.09375 to 0.09375
- w_out: bfloat16 [4, 2048, 4096], P('section', 'mp'), may hold values from -0.125 to 0.125
- vis_gain: float32 [2, 1024], replicated, may hold values from 0.5 to 2
- vis_bias: float32 [2, 1024], replicated, may hold values from -3 to 3
- v_qkv: bfloat16 [3, 1024, 1024], P(None, ('section', 'dp'), 'mp'), may hold values from -0.1875 to 0.1875
- v_out: bfloat16 [1024, 1024], P('mp', ('section', 'dp')), may hold values from -0.1875 to 0.1875
- v_up: bfloat16 [1024, 4096], P(('section', 'dp'), 'mp'), may hold values from -0.1875 to 0.1875
- v_down: bfloat16 [4096, 1024], P('mp', ('section', 'dp')), may hold values from -0.09375 to 0.09375
- v_proj: bfloat16 [4096, 4096], P(('section', 'dp'), 'mp'), may hold values from -0.09375 to 0.09375
Outputs:
- hidden: bfloat16 [4, 1024, 4096], P('section', ('dp', 'mp'))
- token_weight: float32 [4, 1024], P('section', ('dp', 'mp'))
The draws below stay inside these ranges and needn't reach their ends.
Inputs may be any that keep to these rules, and one draw needn't show every extreme that they name: `tile_batch`: in every data-parallel index, the 2 tiles of each section index go 1 to each of two different micro-batches; one micro-batch receives 1 tiles from every section index. `tile_offset`: offsets are multiples of 64; the runs of one sequence never intersect. `loss_mask`: the first position of every sequence is a one.
All inputs are finite; a program needn't handle non-finite values.
Results may differ from the reference program's by a relative error of at most 0.025.
Values may be sent and summed in bfloat16 or wider, within the bound.
A program may use at most 192 MiB of HBM per device.

```python
import math
import jax
import jax.numpy as jnp
import numpy as np
from jax import lax

D = 4096
QH = 16
KVH = 4
HD = 128
VD = 1024
VH = 16
VHD = 64
VFF = 4096
GRID = 16
PATCH = 256
POOL = 64
L = 512
TILES_G = 2
CAP = 1
MICRO = 4
TILES = 16
N_SECTION = 4
N_DP = 2
N_MP = 4


def tile_plan(key):
    base_key = jax.random.fold_in(key, 7)
    target_key, second_key, order_key, slot_key = jax.random.split(base_key, 4)
    tile_count = N_SECTION * TILES_G
    target = jax.random.randint(target_key, (N_DP, 1), 0, MICRO)
    moved = jax.random.randint(second_key, (N_DP, N_SECTION), 1, MICRO)
    second = jnp.mod(target + moved, MICRO)
    orders = jax.vmap(lambda item_key: jax.random.permutation(item_key, TILES_G))(jax.random.split(order_key, N_DP * N_SECTION))
    orders = orders.reshape(N_DP, N_SECTION, TILES_G)
    batches = jnp.where(orders < CAP, target[:, :, None], second[:, :, None]).reshape(N_DP, tile_count)
    tile_ids = jnp.arange(tile_count, dtype=jnp.int32)
    earlier = tile_ids[None, :] < tile_ids[:, None]
    same = batches[:, :, None] == batches[:, None, :]
    ranks = jnp.sum((same & earlier[None, :, :]).astype(jnp.int32), axis=2)
    slot_total = L // POOL
    slot_perm = jax.vmap(lambda item_key: jax.random.permutation(item_key, slot_total))(jax.random.split(slot_key, N_DP * MICRO))
    slot_perm = slot_perm.reshape(N_DP, MICRO * slot_total)
    offsets = POOL * jnp.take_along_axis(slot_perm, batches * slot_total + ranks, axis=1)
    return (batches.astype(jnp.int32), offsets.astype(jnp.int32))


def draw_tile_batch(key, part):
    batches, offsets = tile_plan(key)
    return batches


def draw_tile_offset(key, part):
    batches, offsets = tile_plan(key)
    return offsets


def draw_loss_mask(key, part):
    seq_count = MICRO * N_DP
    seq_index = jnp.arange(seq_count, dtype=jnp.int32)
    threshold = 250 + 500 * seq_index // max(seq_count - 1, 1)
    rolls = jax.random.randint(jax.random.fold_in(key, 5), (seq_count, L), 0, 1000)
    marked = (rolls < threshold[:, None]).astype(jnp.int32)
    leading = (jnp.arange(L) == 0).astype(jnp.int32)
    marked = jnp.maximum(marked, leading[None, :])
    return marked.reshape(MICRO, N_DP * L)


def gain_values(key, shape):
    return jax.random.uniform(key, shape, jnp.float32, 0.5, 1.5)


def draw_attn_gain(key, part):
    return gain_values(jax.random.fold_in(key, 3), (N_SECTION, D))


def draw_vis_gain(key, part):
    return gain_values(jax.random.fold_in(key, 4), (2, VD))


def shard_levels(stream_key, extent, pieces, low, high):
    level, own = 1.0, jax.random.fold_in(stream_key, 6)
    for axis_at, shards_of in pieces:
        heights = jnp.exp(jax.random.uniform(jax.random.fold_in(own, axis_at), (shards_of,), jnp.float32, low / len(pieces), high / len(pieces)))
        level = level * jnp.repeat(heights, extent[axis_at] // shards_of).reshape([-1 if axis == axis_at else 1 for axis in range(len(extent))])
    return level


def split_up(number_of, total, bound, slope):
    loads = [(1 << 20) // math.isqrt(grade ** slope) + 1 for grade in range(2, number_of + 1)]
    surplus, given = total - bound - (number_of - 1), [1] * (number_of - 1)
    while surplus > 0:
        free = [i for i in range(number_of - 1) if given[i] < bound]
        pool, remaining = sum([loads[i] for i in free]), surplus
        for i in free:
            extra = min(bound - given[i], max(1, remaining * loads[i] // pool), surplus)
            given[i] = given[i] + extra
            surplus = surplus - extra
    return np.array([bound] + given)


def uneven(rng, count, total, reach, slope):
    if count == 2:
        one = jax.random.randint(rng, (), max(1, total - reach), min(reach, total - 1) + 1)
        return jnp.stack([one, total - one])
    sizes = jnp.asarray(split_up(count, total, reach, slope), jnp.int32)
    twos = (count - 1) // 2
    source_of, sink = sizes[1:1 + 2 * twos:2], sizes[2:2 + 2 * twos:2]
    margin = jnp.minimum(source_of - 1, reach - sink)
    shifted = jax.random.randint(jax.random.fold_in(rng, 1), (twos,), 0, 1 << 20) % (margin + 1)
    sizes = sizes.at[1:1 + 2 * twos:2].set(source_of - shifted).at[2:2 + 2 * twos:2].set(sink + shifted)
    return sizes[jax.random.permutation(jax.random.fold_in(rng, 2), count)]


def normal_values(stream_key, shape, scale, bound, pieces=(), kind=jnp.bfloat16):
    values = jax.random.normal(stream_key, shape, jnp.float32) * scale
    if len(pieces) > 0:
        values = shard_levels(stream_key, shape, pieces, -0.22, 0.18) * values
    return jnp.clip(values, min=-bound, max=bound).astype(kind)


def setup_inputs(seed: int = 0) -> dict:
    key_list = jax.random.split(jax.random.key(seed), 18)
    return {
        "text": normal_values(key_list[0], (MICRO, N_DP * L, D), 1.0, 6.0, ((0, 4), (1, 8))),
        "patches": normal_values(key_list[1], (TILES * PATCH, VD), 1.0, 6.0, ((0, 8),)),
        "segments": jax.vmap(lambda own: jnp.searchsorted(jnp.cumsum(uneven(own, 4, L, L // 2, 2)), jnp.arange(L), side="right"))(jax.random.split(key_list[2], MICRO * N_DP)).reshape((MICRO, N_DP, L)).astype(jnp.int32),
        "loss_mask": draw_loss_mask(jax.random.fold_in(key_list[17], 71), 0),
        "tile_batch": draw_tile_batch(jax.random.fold_in(key_list[17], 71), 0),
        "tile_offset": draw_tile_offset(jax.random.fold_in(key_list[17], 71), 0),
        "attn_gain": draw_attn_gain(jax.random.fold_in(key_list[17], 71), 0),
        "w_query": normal_values(key_list[7], (N_SECTION, D, QH * HD), D ** -0.5, 0.09375, ((0, 4), (2, 4))),
        "w_kv": normal_values(key_list[8], (N_SECTION, 2, D, KVH * HD), D ** -0.5, 0.09375, ((0, 4), (3, 4))),
        "w_out": normal_values(key_list[9], (N_SECTION, QH * HD, D), (QH * HD) ** -0.5, 0.125, ((0, 4), (1, 4))),
        "vis_gain": draw_vis_gain(jax.random.fold_in(key_list[17], 71), 0),
        "vis_bias": normal_values(key_list[11], (2, VD), 0.5, 3.0, (), jnp.float32),
        "v_qkv": normal_values(key_list[12], (3, VD, VD), VD ** -0.5, 0.1875, ((1, 8), (2, 4))),
        "v_out": normal_values(key_list[13], (VD, VD), VD ** -0.5, 0.1875, ((0, 4), (1, 8))),
        "v_up": normal_values(key_list[14], (VD, VFF), VD ** -0.5, 0.1875, ((0, 8), (1, 4))),
        "v_down": normal_values(key_list[15], (VFF, VD), VFF ** -0.5, 0.09375, ((0, 4), (1, 8))),
        "v_proj": normal_values(key_list[16], (4 * VD, D), (4 * VD) ** -0.5, 0.09375, ((0, 8), (1, 4))),
    }


EPS = 1e-05
ROPE_BASE = 500000.0
BLOCKED = -1e+30

def layer_norm(values, gain, bias):
    wide = values.astype(jnp.float32)
    center = wide - lax.optimization_barrier(jnp.mean(wide, axis=-1, keepdims=True))
    spread = lax.optimization_barrier(jnp.mean(center * center, axis=-1, keepdims=True))
    return (center * lax.rsqrt(spread + EPS) * gain + bias).astype(jnp.bfloat16)

def rms_norm(values, gain):
    wide = values.astype(jnp.float32)
    power = lax.optimization_barrier(jnp.mean(wide * wide, axis=-1, keepdims=True))
    return (wide * lax.rsqrt(power + EPS) * gain).astype(jnp.bfloat16)

def rotate(values, positions):
    half_width = values.shape[-1] // 2
    freqs = ROPE_BASE ** (-2.0 * jnp.arange(half_width, dtype=jnp.float32) / values.shape[-1])
    angles = positions.astype(jnp.float32)[:, None] * freqs[None, :]
    cosine = jnp.cos(angles)[:, None, :]
    sinus_part = jnp.sin(angles)[:, None, :]
    first_half = values[..., :half_width]
    second_half = values[..., half_width:]
    return jnp.concatenate([first_half * cosine - second_half * sinus_part, second_half * cosine + first_half * sinus_part], axis=-1)

def split_sum(left, right):
    row_count = left.shape[0]
    block_width = left.shape[1] // N_MP
    left_blocks = left.reshape(row_count, N_MP, block_width).astype(jnp.float32)
    right_blocks = right.reshape(N_MP, block_width, right.shape[1]).astype(jnp.float32)
    partials = jnp.einsum('rgk,gkn->grn', left_blocks, right_blocks)
    rounded = lax.optimization_barrier(partials.astype(jnp.bfloat16))
    return lax.optimization_barrier(jnp.sum(rounded.astype(jnp.float32), axis=0))

def pixel_shuffle(states):
    tile_count = states.shape[0] // PATCH
    side_half = GRID // 2
    width = states.shape[1]
    arranged = states.reshape(tile_count, side_half, 2, side_half, 2, width)
    return arranged.transpose(0, 1, 3, 2, 4, 5).reshape(tile_count * side_half * side_half, 4 * width)

def encode_group(block, vis_gain, vis_bias, v_qkv, v_out, v_up, v_down, v_proj):
    tile_count = block.shape[0] // PATCH
    normed = layer_norm(block, vis_gain[0], vis_bias[0])
    projected = [jnp.dot(normed, v_qkv[index], preferred_element_type=jnp.float32).astype(jnp.bfloat16).reshape(tile_count, PATCH, VH, VHD) for index in range(3)]
    scores = jnp.einsum('tqhd,tkhd->thqk', projected[0].astype(jnp.float32), projected[1].astype(jnp.float32)) * VHD ** (-0.5)
    probs = jax.nn.softmax(scores, axis=-1).astype(jnp.bfloat16)
    mixed = jnp.einsum('thqk,tkhd->tqhd', probs.astype(jnp.float32), projected[2].astype(jnp.float32)).astype(jnp.bfloat16).reshape(tile_count * PATCH, VD)
    residual = (block.astype(jnp.float32) + split_sum(mixed, v_out)).astype(jnp.bfloat16)
    normed_two = layer_norm(residual, vis_gain[1], vis_bias[1])
    inner = jax.nn.gelu(jnp.dot(normed_two, v_up, preferred_element_type=jnp.float32), approximate=False).astype(jnp.bfloat16)
    states = (residual.astype(jnp.float32) + split_sum(inner, v_down)).astype(jnp.bfloat16)
    return jnp.dot(pixel_shuffle(states), v_proj, preferred_element_type=jnp.float32).astype(jnp.bfloat16)

def decoder_layer(state, segment_ids, gain, w_query, w_kv, w_out):
    length = state.shape[0]
    positions = jnp.arange(length, dtype=jnp.int32)
    normed = rms_norm(state, gain)
    query = rotate(jnp.dot(normed, w_query, preferred_element_type=jnp.float32).reshape(length, QH, HD), positions).astype(jnp.bfloat16)
    keyed = rotate(jnp.dot(normed, w_kv[0], preferred_element_type=jnp.float32).reshape(length, KVH, HD), positions).astype(jnp.bfloat16)
    valued = jnp.dot(normed, w_kv[1], preferred_element_type=jnp.float32).astype(jnp.bfloat16).reshape(length, KVH, HD)
    grouped = query.reshape(length, KVH, QH // KVH, HD).astype(jnp.float32)
    scores = jnp.einsum('qkgd,skd->kgqs', grouped, keyed.astype(jnp.float32)) * HD ** (-0.5)
    allowed = (segment_ids[:, None] == segment_ids[None, :]) & (positions[None, :] <= positions[:, None])
    scores = jnp.where(allowed, scores, BLOCKED)
    probs = jax.nn.softmax(scores, axis=-1).astype(jnp.bfloat16)
    mixed = jnp.einsum('kgqs,skd->qkgd', probs.astype(jnp.float32), valued.astype(jnp.float32)).astype(jnp.bfloat16).reshape(length, QH * HD)
    return (state.astype(jnp.float32) + split_sum(mixed, w_out)).astype(jnp.bfloat16)

def reference(text, patches, segments, loss_mask, tile_batch, tile_offset, attn_gain, w_query, w_kv, w_out, vis_gain, vis_bias, v_qkv, v_out, v_up, v_down, v_proj):
    group_count = N_SECTION * N_DP
    grouped = patches.reshape(group_count, TILES_G * PATCH, VD)
    embedded = lax.map(lambda block: encode_group(block, vis_gain, vis_bias, v_qkv, v_out, v_up, v_down, v_proj), grouped)
    per_tile = embedded.reshape(N_SECTION, N_DP, TILES_G, POOL, D).transpose(1, 0, 2, 3, 4).reshape(N_DP, N_SECTION * TILES_G, POOL, D)
    states = text.reshape(MICRO, N_DP, L, D)
    places = tile_offset[:, :, None] + jnp.arange(POOL, dtype=jnp.int32)[None, None, :]
    dp_ids = jnp.broadcast_to(jnp.arange(N_DP, dtype=jnp.int32)[:, None, None], places.shape)
    micro_ids = jnp.broadcast_to(tile_batch[:, :, None], places.shape)
    states = states.at[micro_ids, dp_ids, places].set(per_tile)
    flat_states = states.reshape(MICRO * N_DP, L, D)
    flat_segments = segments.reshape(MICRO * N_DP, L)

    def run_sequence(pair):
        state, segment_ids = pair
        for layer_index in range(N_SECTION):
            state = decoder_layer(state, segment_ids, attn_gain[layer_index], w_query[layer_index], w_kv[layer_index], w_out[layer_index])
        return state
    hidden = lax.map(run_sequence, (flat_states, flat_segments)).reshape(MICRO, N_DP * L, D)
    weights = loss_mask.astype(jnp.float32)
    token_weight = weights * (MICRO * N_DP * L) / jnp.sum(weights)
    return (hidden, token_weight)
```

```python
import functools

import jax
import jax.numpy as jnp
from jax import lax
from jax.experimental import pallas as pl
from jax.experimental.pallas import tpu as pltpu
from jax.sharding import PartitionSpec as P

HD = 128
VHD = 64
GRID = 16
PATCH = 256
POOL = 64


EPS = 1e-05
ROPE_BASE = 500000.0
BLOCKED = -1e30
PAIR = 2
PIECES = 4
MESH = pl.DeviceIdType.MESH


def layer_norm(values, gain, bias):
    wide = values.astype(jnp.float32)
    center = wide - jnp.mean(wide, axis=-1, keepdims=True)
    spread = jnp.mean(center * center, axis=-1, keepdims=True)
    return (center * lax.rsqrt(spread + EPS) * gain + bias).astype(jnp.bfloat16)


def mirrored(value, bit, axis):
    count = lax.axis_size(axis)
    return lax.ppermute(value, axis, [(at, at ^ bit) for at in range(count)])


def shifted(value, step, axis):
    count = lax.axis_size(axis)
    return lax.ppermute(value, axis, [(at, (at + step) % count) for at in range(count)])


def spread_pairs(piece, axis, low=1):
    count = lax.axis_size(axis)
    held = {0: piece}
    bit = count // 2
    while bit >= low:
        for slot in list(held):
            held[slot | bit] = mirrored(held[slot], bit, axis)
        bit //= 2
    return held


def spread_ring(piece, axis):
    count = lax.axis_size(axis)
    held = {0: piece}
    up = down = piece
    for step in range(1, (count - 1) // 2 + 1):
        up, down = shifted(up, 1, axis), shifted(down, -1, axis)
        held[count - step], held[step] = up, down
    if count % 2 == 0:
        half = piece.shape[0] // 2
        held[count // 2] = jnp.concatenate(
            [shifted(up[:half], 1, axis), shifted(down[half:], -1, axis)], axis=0
        )
    return held


def in_order(held, places):
    stacked = jnp.stack([held[slot] for slot in range(len(held))])
    return [lax.dynamic_index_in_dim(stacked, place, 0, keepdims=False) for place in places]


def gather_pairs(piece, axis, dim=0):
    at = lax.axis_index(axis)
    held = spread_pairs(piece, axis)
    return jnp.concatenate(in_order(held, [at ^ k for k in range(len(held))]), axis=dim)


def gather_ring(piece, axis, dim=0):
    at = lax.axis_index(axis)
    held = spread_ring(piece, axis)
    count = len(held)
    return jnp.concatenate(in_order(held, [(k - at) % count for k in range(count)]), axis=dim)


def gather_weights(piece, dim=0):
    return gather_ring(gather_pairs(piece, "dp", dim), "section", dim)


def scatter_slots(partial_value, axis="mp"):
    count = lax.axis_size(axis)
    current = partial_value
    bit = 1
    while bit < count:
        half = current.shape[0] // 2
        arrived = mirrored(current[half:].astype(jnp.bfloat16), bit, axis)
        current = current[:half].astype(jnp.float32) + arrived.astype(jnp.float32)
        bit *= 2
    return current


def slot_order(count):
    order = [0]
    bit = count // 2
    while bit >= 1:
        order = order + [slot | bit for slot in order]
        bit //= 2
    return order


def own_slots(values, part_at, axis="mp"):
    count = lax.axis_size(axis)
    rows = values.shape[0] // count
    return jnp.concatenate(
        [
            lax.dynamic_slice_in_dim(values, (part_at ^ slot) * rows, rows, 0)
            for slot in slot_order(count)
        ],
        axis=0,
    )


def encode_tiles(patches, vis_gain, vis_bias, qkv_full, out_full, up_full, down_full, part_at):
    tile_count = patches.shape[0] // PATCH
    local_width = qkv_full.shape[1] // 3
    head_count = local_width // VHD
    normed = layer_norm(patches, vis_gain[0], vis_bias[0])
    projected = [
        jnp.dot(
            normed,
            qkv_full[:, index * local_width : (index + 1) * local_width],
            preferred_element_type=jnp.float32,
        )
        .astype(jnp.bfloat16)
        .reshape(tile_count, PATCH, head_count, VHD)
        for index in range(3)
    ]
    scores = jnp.einsum(
        "tqhd,tkhd->thqk", projected[0], projected[1], preferred_element_type=jnp.float32
    ) * VHD ** (-0.5)
    probs = jax.nn.softmax(scores, axis=-1).astype(jnp.bfloat16)
    mixed = (
        jnp.einsum("thqk,tkhd->tqhd", probs, projected[2], preferred_element_type=jnp.float32)
        .astype(jnp.bfloat16)
        .reshape(tile_count * PATCH, local_width)
    )
    mixed = own_slots(mixed, part_at)
    attended = scatter_slots(
        jnp.dot(mixed, out_full, preferred_element_type=jnp.float32).astype(jnp.bfloat16)
    )
    rows = attended.shape[0]
    own = lax.dynamic_slice_in_dim(patches, part_at * rows, rows, 0)
    residual = (own.astype(jnp.float32) + attended).astype(jnp.bfloat16)
    held = spread_pairs(layer_norm(residual, vis_gain[1], vis_bias[1]), "mp")
    normed_two = jnp.concatenate([held[slot] for slot in slot_order(len(held))], axis=0)
    inner = jax.nn.gelu(
        jnp.dot(normed_two, up_full, preferred_element_type=jnp.float32), approximate=False
    ).astype(jnp.bfloat16)
    fed = scatter_slots(
        jnp.dot(inner, down_full, preferred_element_type=jnp.float32).astype(jnp.bfloat16)
    )
    states = (residual.astype(jnp.float32) + fed).astype(jnp.bfloat16)
    width = states.shape[1]
    arranged = states.reshape(rows // (2 * GRID), 2, GRID // 2, 2, width)
    return arranged.transpose(0, 2, 1, 3, 4).reshape(rows // 4, 4 * width)


def decoder_kernel(
    sections,
    parts,
    seqs,
    pick_ref,
    seg_row_ref,
    seg_col_ref,
    gain_ref,
    cos_ref,
    sin_ref,
    image_own_ref,
    image_other_ref,
    text_ref,
    *refs,
):
    groups = parts // PAIR
    weight_refs = refs[: len(refs) - 26]
    (
        out_ref,
        w_in,
        w_out,
        arrived,
        normed,
        query,
        keyed,
        valued,
        bias,
        mixed,
        part,
        kept,
        give,
        take,
        done,
        home,
        w_sem,
        text_send,
        text_recv,
        n_send,
        n_recv,
        rs_send,
        rs_recv,
        hop_send,
        hop_recv,
        home_recv,
    ) = refs[len(refs) - 26 :]
    section = lax.axis_index("section")
    place = lax.axis_index("mp")
    low = lax.rem(place, PAIR)
    group = place // PAIR
    partner = group * PAIR + (1 - low)
    items, own, width = arrived.shape
    chunk = PAIR * own
    piece = width // PIECES
    kv_width = keyed.shape[1]
    pair_heads = kv_width // HD
    heads = query.shape[0]
    each = heads // pair_heads
    last = sections - 1

    text_group = lax.rem(section, groups)
    text_item = (section // groups) * parts + place

    def text_copy(half):
        return pltpu.make_async_remote_copy(
            src_ref=text_ref.at[0, pl.ds(half * own, own)],
            dst_ref=arrived.at[text_item],
            send_sem=text_send.at[half],
            recv_sem=text_recv.at[text_item],
            device_id={"section": 0, "mp": text_group * PAIR + half},
            device_id_type=MESH,
        )

    for half in range(PAIR):
        here = (section == 0) & (place == text_group * PAIR + half)

        @pl.when(here)
        def _():
            pltpu.make_async_copy(
                text_ref.at[0, pl.ds(half * own, own)],
                arrived.at[text_item],
                text_recv.at[text_item],
            ).start()

        @pl.when(jnp.logical_not(here))
        def _():
            text_copy(half).start()

    in_loads, out_loads = weight_loads(weight_refs, w_in, w_out, groups)
    copies = [
        pltpu.make_async_copy(source, target, w_sem.at[at])
        for at, (source, target) in enumerate(in_loads + out_loads)
    ]
    for copy in copies:
        copy.start()
    keyed[...] = jnp.zeros_like(keyed)
    valued[...] = jnp.zeros_like(valued)
    first_count = len(in_loads)

    def one_item(item, carry):
        seq = item // parts
        at = lax.rem(item, parts)
        rows = pl.ds(pl.multiple_of(at * chunk, chunk), chunk)
        own_rows = pl.ds(pl.multiple_of(low * own, own), own)
        other_rows = pl.ds(pl.multiple_of((1 - low) * own, own), own)

        @pl.when(section == 0)
        def _():
            pltpu.make_async_copy(arrived.at[item], arrived.at[item], text_recv.at[item]).wait()
            cover = jnp.full((own, 1), pick_ref[item, 2], jnp.int32) > 0
            span = image_own_ref.shape[-1]
            for g in range(groups):
                for ref, lane in ((image_own_ref, low), (image_other_ref, 1 - low)):
                    cols = pl.ds(pl.multiple_of((g * PAIR + lane) * span, span), span)
                    arrived[item, :, cols] = jnp.where(
                        cover, ref[pick_ref[item, 0], g, pick_ref[item, 1]], arrived[item, :, cols]
                    )

        @pl.when(section > 0)
        def _():
            for t in range(PIECES):
                ref = arrived.at[item, :, pl.ds(t * piece, piece)]
                pltpu.make_async_copy(ref, ref, hop_recv.at[item, t]).wait()

        for r in range(0, own, 16):
            wide = arrived[item, r : r + 16, :].astype(jnp.float32)
            power = jnp.mean(wide * wide, axis=-1, keepdims=True)
            to = pl.ds(pl.multiple_of(low * own + r, 16), 16)
            normed[item, to, :] = (wide * lax.rsqrt(power + EPS) * gain_ref[...]).astype(
                jnp.bfloat16
            )
        n_copy = pltpu.make_async_remote_copy(
            src_ref=normed.at[item, own_rows],
            dst_ref=normed.at[item, own_rows],
            send_sem=n_send.at[item],
            recv_sem=n_recv.at[item],
            device_id={"mp": partner},
            device_id_type=MESH,
        )
        n_copy.start()
        allowed = (seg_col_ref[seq, rows, :] == seg_row_ref[seq]) & (
            lax.broadcasted_iota(jnp.int32, bias.shape, 1)
            <= lax.broadcasted_iota(jnp.int32, bias.shape, 0) + at * chunk
        )
        bias[...] = jnp.where(allowed, 0.0, BLOCKED)

        @pl.when(item == 0)
        def _():
            for copy in copies[:first_count]:
                copy.wait()

        n_copy.wait_recv()

        cosine, sinus = cos_ref[rows, :], sin_ref[rows, :]

        def turned(col):
            made = jnp.dot(
                normed[item],
                w_in[:, pl.ds(pl.multiple_of(col, kv_width), kv_width)],
                preferred_element_type=jnp.float32,
            )
            outs = []
            for h in range(pair_heads):
                head = made[:, h * HD : (h + 1) * HD]
                outs.append(
                    (head * cosine + pltpu.roll(head, HD // 2, 1) * sinus).astype(jnp.bfloat16)
                )
            return outs

        def query_tile(tile, c):
            for h, value in enumerate(turned(tile * kv_width)):
                query[tile * pair_heads + h] = value
            return c

        lax.fori_loop(0, heads // pair_heads, query_tile, 0)
        for h, value in enumerate(turned(heads * HD)):
            keyed[rows, h * HD : (h + 1) * HD] = value
        valued[rows, :] = jnp.dot(
            normed[item],
            w_in[:, heads * HD + kv_width :],
            preferred_element_type=jnp.float32,
        ).astype(jnp.bfloat16)

        for h in range(heads):
            kv = slice((h // each) * HD, (h // each + 1) * HD)
            scores = (
                lax.dot_general(
                    query[h],
                    keyed[:, kv],
                    (((1,), (1,)), ((), ())),
                    preferred_element_type=jnp.float32,
                )
                * HD ** (-0.5)
                + bias[...]
            )
            high = jnp.max(scores, axis=-1, keepdims=True)
            grown = jnp.exp(scores - high)
            probs = (grown / jnp.sum(grown, axis=-1, keepdims=True)).astype(jnp.bfloat16)
            mixed[:, h * HD : (h + 1) * HD] = jnp.dot(
                probs, valued[:, kv], preferred_element_type=jnp.float32
            ).astype(jnp.bfloat16)

        @pl.when(item == 0)
        def _():
            for copy in copies[first_count:]:
                copy.wait()

        def give_copy(t):
            return pltpu.make_async_remote_copy(
                src_ref=give.at[item, :, pl.ds(t * piece, piece)],
                dst_ref=take.at[item, :, pl.ds(t * piece, piece)],
                send_sem=rs_send.at[item, t],
                recv_sem=rs_recv.at[item, t],
                device_id={"mp": partner},
                device_id_type=MESH,
            )

        for t in range(PIECES):
            cols = slice(t * piece, (t + 1) * piece)
            part[...] = jnp.dot(mixed[...], w_out[:, cols], preferred_element_type=jnp.float32)
            give[item, :, cols] = part[other_rows, :].astype(jnp.bfloat16)
            give_copy(t).start()
            kept[:, cols] = part[own_rows, :] + arrived[item, :, cols].astype(jnp.float32)

        goal = seq * groups + group
        stays = (section == last) & (goal == last) & (at == place)
        for t in range(PIECES):
            cols = slice(t * piece, (t + 1) * piece)
            give_copy(t).wait_recv()
            done[item, :, cols] = (
                kept[:, cols] + take[item, :, cols].astype(jnp.float32)
            ).astype(jnp.bfloat16)

            @pl.when(section < last)
            def _():
                hop_copy(item, t).start()

            @pl.when((section == last) & jnp.logical_not(stays))
            def _():
                home_copy(item, t).start()

            @pl.when(stays)
            def _():
                home[own_rows, cols] = done[item, :, cols]

        return carry

    def hop_copy(item, t):
        return pltpu.make_async_remote_copy(
            src_ref=done.at[item, :, pl.ds(t * piece, piece)],
            dst_ref=arrived.at[item, :, pl.ds(t * piece, piece)],
            send_sem=hop_send.at[item, t],
            recv_sem=hop_recv.at[item, t],
            device_id={"section": lax.rem(section + 1, sections)},
            device_id_type=MESH,
        )

    def home_copy(item, t):
        return pltpu.make_async_remote_copy(
            src_ref=done.at[item, :, pl.ds(t * piece, piece)],
            dst_ref=home.at[pl.ds(pl.multiple_of(low * own, own), own), pl.ds(t * piece, piece)],
            send_sem=hop_send.at[item, t],
            recv_sem=home_recv.at[low, t],
            device_id={"section": (item // parts) * groups + group, "mp": lax.rem(item, parts)},
            device_id_type=MESH,
        )

    lax.fori_loop(0, items, one_item, 0)

    for half in range(PAIR):
        here = (section == 0) & (place == text_group * PAIR + half)

        @pl.when(jnp.logical_not(here))
        def _():
            text_copy(half).wait_send()

    def drain(item, carry):
        n_ref = normed.at[item, pl.ds(0, own)]
        pltpu.make_async_copy(n_ref, n_ref, n_send.at[item]).wait()
        goal = (item // parts) * groups + group
        stays = (section == last) & (goal == last) & (lax.rem(item, parts) == place)
        for t in range(PIECES):
            ref = give.at[item, :, pl.ds(t * piece, piece)]
            pltpu.make_async_copy(ref, ref, rs_send.at[item, t]).wait()

            @pl.when(jnp.logical_not(stays))
            def _():
                ref = done.at[item, :, pl.ds(t * piece, piece)]
                pltpu.make_async_copy(ref, ref, hop_send.at[item, t]).wait()

        return carry

    lax.fori_loop(0, items, drain, 0)
    for half in range(PAIR):
        sender = lax.rem(section, groups) * PAIR + half

        @pl.when(jnp.logical_not((section == last) & (place == sender)))
        def _():
            for t in range(PIECES):
                ref = home.at[pl.ds(half * own, own), pl.ds(t * piece, piece)]
                pltpu.make_async_copy(ref, ref, home_recv.at[half, t]).wait()

    out_ref[0] = home[...]


def weight_loads(refs, w_in, w_out, groups):
    query_ref, kv_ref, out_ref = refs[:3]
    query_span, kv_span, out_span = query_ref.shape[2], kv_ref.shape[3], out_ref.shape[1]
    depth = w_in.shape[0]
    keys_at, values_at = query_span * groups, (query_span + kv_span) * groups
    even = lax.rem(lax.axis_index("dp"), 2)
    in_loads = [
        (query_ref.at[0], w_in.at[:, pl.ds(0, query_span)]),
        (kv_ref.at[0, 0], w_in.at[:, pl.ds(keys_at, kv_span)]),
        (kv_ref.at[0, 1], w_in.at[:, pl.ds(values_at, kv_span)]),
    ]
    out_loads = [(out_ref.at[0], w_out.at[pl.ds(0, out_span)])]
    sets = refs[3:]
    each = len(sets) // max(groups - 1, 1)
    for other in range(1, groups):
        pieces = sets[(other - 1) * each : other * each]
        for half, at in ((pieces[: each // 2], even), (pieces[each // 2 :], 1 - even)):
            rows_in = half[0].shape[0]
            for order, ref in enumerate(half[:-1]):
                start = pl.multiple_of(at * (depth // 2) + order * rows_in, rows_in)
                rows = pl.ds(start, rows_in)
                for low, span, to in (
                    (0, query_span, other * query_span),
                    (query_span, kv_span, keys_at + other * kv_span),
                    (query_span + kv_span, kv_span, values_at + other * kv_span),
                ):
                    in_loads.append((ref.at[:, pl.ds(low, span)], w_in.at[rows, pl.ds(to, span)]))
            rows_out = half[-1].shape[0]
            start = pl.multiple_of(other * out_span + at * rows_out, rows_out)
            out_loads.append((half[-1], w_out.at[pl.ds(start, rows_out)]))
    return in_loads, out_loads


def run_decoder(text, image_own, image_other, pick, segs, gain, cosine, sinus, weights, sections, parts):
    seqs, length = segs.shape
    width = text.shape[2]
    chunk = text.shape[1]
    own = chunk // PAIR
    items = seqs * parts
    groups = parts // PAIR
    query_width, kv_width = weights[0].shape[2] * groups, weights[1].shape[3] * groups
    joined = query_width + 2 * kv_width
    loads = 4 + (len(weights) - 3) * 3
    vmem = pl.BlockSpec(memory_space=pltpu.VMEM)
    hbm = pl.BlockSpec(memory_space=pl.ANY)
    smem = pl.BlockSpec(memory_space=pltpu.SMEM)
    dma = pltpu.SemaphoreType.DMA
    bf = jnp.bfloat16
    return pl.pallas_call(
        functools.partial(decoder_kernel, sections, parts, seqs),
        out_shape=jax.ShapeDtypeStruct(text.shape, text.dtype),
        in_specs=[smem] + [vmem] * 7 + [hbm] * (1 + len(weights)),
        out_specs=vmem,
        scratch_shapes=[
            pltpu.VMEM((width, joined), bf),
            pltpu.VMEM((query_width, width), bf),
            pltpu.VMEM((items, own, width), bf),
            pltpu.VMEM((items, chunk, width), bf),
            pltpu.VMEM((query_width // HD, chunk, HD), bf),
            pltpu.VMEM((length, kv_width), bf),
            pltpu.VMEM((length, kv_width), bf),
            pltpu.VMEM((chunk, length), jnp.float32),
            pltpu.VMEM((chunk, query_width), bf),
            pltpu.VMEM((chunk, width // PIECES), jnp.float32),
            pltpu.VMEM((own, width), jnp.float32),
            pltpu.VMEM((items, own, width), bf),
            pltpu.VMEM((items, own, width), bf),
            pltpu.VMEM((items, own, width), bf),
            pltpu.VMEM((chunk, width), bf),
            dma((loads,)),
            dma((PAIR,)),
            dma((items,)),
            dma((items,)),
            dma((items,)),
            dma((items, PIECES)),
            dma((items, PIECES)),
            dma((items, PIECES)),
            dma((items, PIECES)),
            dma((PAIR, PIECES)),
        ],
        compiler_params=pltpu.CompilerParams(
            has_side_effects=True, vmem_limit_bytes=63 * 1024 * 1024
        ),
        cost_estimate=pl.CostEstimate(
            flops=2 * items * chunk * width * (joined + query_width),
            bytes_accessed=2 * width * (joined + query_width),
            transcendentals=0,
        ),
    )(
        pick,
        segs[:, None, :],
        segs[:, :, None],
        gain,
        cosine,
        sinus,
        image_own,
        image_other,
        text,
        *weights,
    )


def other_half(value, at):
    rows = value.shape[0] // 2
    return lax.dynamic_slice_in_dim(value, at * rows, rows, 0)


def shards(
    text,
    patches,
    segments,
    loss_mask,
    tile_batch,
    tile_offset,
    attn_gain,
    w_query,
    w_kv,
    w_out,
    vis_gain,
    vis_bias,
    v_qkv,
    v_out,
    v_up,
    v_down,
    v_proj,
):
    sections = lax.axis_size("section")
    replicas = lax.axis_size("dp")
    parts = lax.axis_size("mp")
    groups = parts // PAIR
    section_at = lax.axis_index("section")
    replica_at = lax.axis_index("dp")
    part_at = lax.axis_index("mp")
    low_at = part_at % PAIR
    group_at = part_at // PAIR
    length = segments.shape[2]

    qkv_full = gather_weights(jnp.concatenate([v_qkv[0], v_qkv[1], v_qkv[2]], axis=1))
    out_full = gather_weights(v_out, 1)
    up_full = gather_weights(v_up)
    down_full = gather_weights(v_down, 1)
    proj_held = spread_ring(gather_pairs(v_proj, "dp"), "section")

    joined = jnp.concatenate([w_query[0], w_kv[0, 0], w_kv[0, 1]], axis=1)
    even = replica_at % 2
    in_half = other_half(joined, even)
    out_half = other_half(w_out[0], even)
    in_cuts = jnp.split(in_half, 2, axis=0)
    sent = in_cuts + [out_half]
    other_sets = []
    for step in range(1, groups):
        hops = [(at, (at + step * PAIR) % parts) for at in range(parts)]
        first = [lax.ppermute(value, "mp", hops) for value in sent]
        second = [mirrored(value, 1, "dp") for value in first]
        other_sets.append((first, second))

    seg_held = spread_pairs(segments[0, 0], "section")
    seg_all = jnp.stack(in_order(seg_held, [section_at ^ k for k in range(sections)]))
    seqs = sections // groups
    seg_mine = jnp.take(seg_all.reshape(seqs, groups, length), group_at, axis=1)
    totals = jnp.sum(loss_mask).reshape(1)
    for axis in ("mp", "dp", "section"):
        bit = 1
        while bit < lax.axis_size(axis):
            totals = totals + mirrored(totals, bit, axis)
            bit *= 2
    scaling = float(sections * replicas * length)
    token_weight = loss_mask.astype(jnp.float32) * scaling / totals.astype(jnp.float32)

    pooled = encode_tiles(
        patches, vis_gain, vis_bias, qkv_full, out_full, up_full, down_full, part_at
    )
    own_rows = pooled.shape[0]
    pooled_all = gather_pairs(pooled, "mp")
    depth = pooled.shape[1] // sections
    image = jnp.zeros((own_rows * parts, v_proj.shape[1]), jnp.float32)
    for step in range(sections):
        start = ((section_at + step) % sections) * depth
        image = image + jnp.dot(
            lax.dynamic_slice_in_dim(pooled_all, start, depth, 1),
            proj_held[step],
            preferred_element_type=jnp.float32,
        )
    image = image.astype(jnp.bfloat16)
    held = spread_pairs(image, "mp", PAIR)
    wide = jnp.stack(
        in_order({k // PAIR: v for k, v in held.items()}, [group_at ^ k for k in range(groups)])
    )
    tiles_here = own_rows * parts // POOL
    landed = [wide] + [lax.ppermute(wide, "section", [(at, 0)]) for at in range(1, sections)]
    image_own = jnp.stack(landed).reshape(sections, groups, tiles_here, POOL, image.shape[1])
    image_other = mirrored(image_own, 1, "mp")

    batch_all = tile_batch[0]
    offset_all = tile_offset[0]
    items = seqs * parts
    item_ids = jnp.arange(items, dtype=jnp.int32)
    item_batch = (item_ids // parts) * groups + group_at
    chunk = text.shape[1]
    item_place = (item_ids % parts) * chunk + low_at * (chunk // PAIR)
    hit = (batch_all[None, :] == item_batch[:, None]) & (
        offset_all[None, :] == item_place[:, None]
    )
    tile_at = jnp.sum(hit * jnp.arange(batch_all.shape[0], dtype=jnp.int32)[None, :], axis=1)
    pick = jnp.stack(
        [tile_at // tiles_here, tile_at % tiles_here, jnp.any(hit, axis=1).astype(jnp.int32)],
        axis=1,
    ).astype(jnp.int32)

    positions = jnp.arange(length, dtype=jnp.int32)
    freqs = ROPE_BASE ** (-2.0 * jnp.arange(HD // 2, dtype=jnp.float32) / HD)
    angles = positions.astype(jnp.float32)[:, None] * freqs[None, :]
    cosine, sinus = jnp.cos(angles), jnp.sin(angles)
    cos_full = jnp.concatenate([cosine, cosine], axis=1)
    sin_full = jnp.concatenate([-sinus, sinus], axis=1)

    weights = [w_query, w_kv, w_out]
    for first, second in other_sets:
        weights = weights + first + second
    hidden = run_decoder(
        text,
        image_own,
        image_other,
        pick,
        seg_mine,
        attn_gain,
        cos_full,
        sin_full,
        weights,
        sections,
        parts,
    )
    return (hidden, token_weight)


def solution(mesh):
    in_specs = (
        P("section", ("dp", "mp"), None),
        P(("section", "dp"), None),
        P("section", "dp", None),
        P("section", ("dp", "mp")),
        P("dp", None),
        P("dp", None),
        P("section", None),
        P("section", None, "mp"),
        P("section", None, None, "mp"),
        P("section", "mp", None),
        P(),
        P(),
        P(None, ("section", "dp"), "mp"),
        P("mp", ("section", "dp")),
        P(("section", "dp"), "mp"),
        P("mp", ("section", "dp")),
        P(("section", "dp"), "mp"),
    )
    out_specs = (P("section", ("dp", "mp"), None), P("section", ("dp", "mp")))
    return jax.shard_map(shards, mesh=mesh, in_specs=in_specs, out_specs=out_specs, check_vma=False)
```

```python
import functools

import jax
import jax.numpy as jnp
from jax import lax
from jax.experimental import pallas as pl
from jax.experimental.pallas import tpu as pltpu
from jax.sharding import PartitionSpec as P

HD = 128
VHD = 64
GRID = 16
PATCH = 256
POOL = 64


EPS = 1e-05
ROPE_BASE = 500000.0
BLOCKED = -1e30
PAIR = 2
PIECES = 4
MESH = pl.DeviceIdType.MESH


def layer_norm(values, gain, bias):
    wide = values.astype(jnp.float32)
    center = wide - jnp.mean(wide, axis=-1, keepdims=True)
    spread = jnp.mean(center * center, axis=-1, keepdims=True)
    return (center * lax.rsqrt(spread + EPS) * gain + bias).astype(jnp.bfloat16)


def remote(source, target, send_sem, recv_sem, **device):
    return pltpu.make_async_remote_copy(
        src_ref=source,
        dst_ref=target,
        send_sem=send_sem,
        recv_sem=recv_sem,
        device_id=device,
        device_id_type=MESH,
    )


def landed(ref, sem):
    pltpu.make_async_copy(ref, ref, sem).wait()


def block_rows(ref, start, count):
    rows = pl.ds(pl.multiple_of(start, 16), count)
    return ref.at[:, rows] if len(ref.shape) == 3 else ref.at[rows]


IN_CHUNKS = 8
OUT_BLOCKS = 16
OUT_SHARED = 3
AHEAD = 1


def vision_kernel(
    sections,
    replicas,
    parts,
    patches_ref,
    gain_ref,
    bias_ref,
    loss_ref,
    seg_ref,
    qkv_src,
    out_src,
    up_src,
    down_src,
    proj_src,
    text_ref,
    wq_ref,
    wkv_ref,
    wo_ref,
    image_own,
    image_other,
    seg_all,
    count_ref,
    text_first,
    other_q,
    other_kv,
    other_o,
    w_qkv,
    w_out,
    w_up,
    w_down,
    w_proj,
    n_one,
    qkv,
    mixed,
    partial,
    pair_in,
    group_out,
    group_in,
    resid,
    n_two,
    inner,
    quads,
    pooled,
    summed,
    far_out,
    far_in,
    wide,
    counts,
    count_src,
    local_sem,
    y_send,
    y_recv,
    up_send,
    up_recv,
    dn_send,
    dn_recv,
    pa_send,
    pa_recv,
    pg_send,
    pg_recv,
    ax_send,
    ax_recv,
    ad_send,
    ad_recv,
    pool_send,
    pool_recv,
    far_send,
    far_recv,
    wide_send,
    wide_recv,
    im_send,
    im_recv,
    io_send,
    io_recv,
    cx_send,
    cx_recv,
    cy_send,
    cy_recv,
    tf_send,
    tf_recv,
    seg_send,
    seg_recv,
    cnt_send,
    cnt_recv,
):
    groups = parts // PAIR
    section = lax.axis_index("section")
    replica = lax.axis_index("dp")
    place = lax.axis_index("mp")
    low = lax.rem(place, PAIR)
    group = place // PAIR
    partner = group * PAIR + (1 - low)
    after = lax.rem(section + 1, sections)
    before = lax.rem(section + sections - 1, sections)
    even = lax.rem(replica, 2)
    mate = replica + 1 - 2 * even
    total_rows, width = patches_ref.shape
    rows = total_rows // parts
    own_rows = pl.ds(pl.multiple_of(place * rows, rows), rows)
    sent = []

    def go(copy):
        copy.start()
        sent.append(copy)

    axes = (("mp", place, parts), ("dp", replica, replicas), ("section", section, sections))

    def count_start(level):
        axis, at, size = axes[level]
        slot = sum(axes[i][2] for i in range(level))
        counts[slot + at] = count_src[level]
        for step in range(1, size):
            go(
                remote(
                    count_src.at[level],
                    counts.at[slot + at],
                    cnt_send.at[slot + step],
                    cnt_recv.at[slot + step],
                    **{axis: lax.rem(at + step, size)},
                )
            )

    def count_finish(level):
        size = axes[level][2]
        slot = sum(axes[i][2] for i in range(level))
        for step in range(1, size):
            landed(count_src.at[level], cnt_recv.at[slot + step])
        value = counts[slot]
        for at in range(1, size):
            value = value + counts[slot + at]
        return value

    first_row = lax.broadcasted_iota(jnp.int32, count_ref.shape, 0) == 0
    count_src[0] = jnp.where(first_row, jnp.broadcast_to(loss_ref[...], count_ref.shape), 0)
    count_start(0)

    for step in range(1, sections):
        go(
            remote(
                seg_ref.at[0],
                seg_all.at[section],
                seg_send.at[step],
                seg_recv.at[step],
                section=lax.rem(section + step, sections),
            )
        )
    seg_here = pltpu.make_async_copy(seg_ref.at[0], seg_all.at[section], seg_recv.at[0])
    seg_here.start()

    weights = [
        (qkv_src, w_qkv, True),
        (out_src, w_out, True),
        (up_src, w_up, True),
        (down_src, w_down, True),
        (proj_src, w_proj, False),
    ]

    def block_at(w, block):
        source, buffer, shared = weights[w]
        count = source.shape[-2]
        if shared:
            return block_rows(buffer, (block * replicas + replica) * count, count)
        return block_rows(buffer, block * count, count)

    def up_copy(w, k, source, target):
        return remote(source, target, up_send.at[w, k], up_recv.at[w, k], section=after)

    def down_copy(w, k, source, target):
        return remote(source, target, dn_send.at[w, k], dn_recv.at[w, k], section=before)

    def share(w, block, source):
        if weights[w][2]:
            for step in range(1, replicas):
                slot = block * replicas + step
                remote(
                    source,
                    block_at(w, block),
                    y_send.at[w, slot],
                    y_recv.at[w, slot],
                    dp=lax.rem(replica + step, replicas),
                ).start()

    def own_start(w):
        source = weights[w][0]
        target = block_at(w, section)
        pltpu.make_async_copy(source, target, local_sem.at[w]).start()

        @pl.when(section < sections - 1)
        def _():
            up_copy(w, 0, source, target).start()

        @pl.when(section > 0)
        def _():
            down_copy(w, 0, source, target).start()

        share(w, section, source)

    def pump(w, k):
        @pl.when(section >= k + 1)
        def _():
            block = section - 1 - k
            ref = block_at(w, block)
            landed(ref, up_recv.at[w, k])

            @pl.when(section < sections - 1)
            def _():
                up_copy(w, k + 1, ref, ref).start()

            share(w, block, ref)

        @pl.when(section + k + 1 <= sections - 1)
        def _():
            block = section + 1 + k
            ref = block_at(w, block)
            landed(ref, dn_recv.at[w, k])

            @pl.when(section > 0)
            def _():
                down_copy(w, k + 1, ref, ref).start()

            share(w, block, ref)

    def pump_from(w, k):
        for at in range(k, sections - 1):
            pump(w, at)

    def all_here(w):
        landed(block_at(w, 0), local_sem.at[w])
        if weights[w][2]:
            for slot in range(sections * replicas):
                if slot % replicas:
                    landed(block_at(w, 0), y_recv.at[w, slot])

    units, chunks, direct = [], [], []
    for step in range(1, groups):
        depth = wq_ref.shape[1] // 2 // IN_CHUNKS
        for c in range(IN_CHUNKS):
            at = pl.ds(pl.multiple_of((even * IN_CHUNKS + c) * depth, depth), depth)
            chunks.append([len(units) + i for i in range(3)])
            units.append((step, wq_ref.at[0, at], other_q.at[step - 1, at]))
            units.append((step, wkv_ref.at[0, 0, at], other_kv.at[step - 1, 0, at]))
            units.append((step, wkv_ref.at[0, 1, at], other_kv.at[step - 1, 1, at]))
    for step in range(1, groups):
        depth = wo_ref.shape[1] // OUT_BLOCKS
        for c in range(OUT_BLOCKS - OUT_SHARED):
            block = even * OUT_SHARED + c if c < OUT_SHARED else OUT_SHARED + c
            at = pl.ds(pl.multiple_of(block * depth, depth), depth)
            chunks.append([len(units)])
            if c >= OUT_SHARED:
                direct.append(len(units))
            units.append((step, wo_ref.at[0, at], other_o.at[step - 1, at]))
    progress = {"x": 0, "y": 0}

    def send_chunks(upto):
        while progress["x"] < min(upto, len(chunks)):
            for u in chunks[progress["x"]]:
                step, source, target = units[u]
                to = lax.rem(group + step, groups) * PAIR + low
                go(remote(source, target, cx_send.at[u], cx_recv.at[u], mp=to))
            progress["x"] += 1

    def forward_chunks(upto):
        while progress["y"] < min(upto, len(chunks)):
            for u in chunks[progress["y"]]:
                step, source, target = units[u]
                landed(target, cx_recv.at[u])
                if u in direct:
                    continue
                go(remote(target, target, cy_send.at[u], cy_recv.at[u], dp=mate))
            progress["y"] += 1

    own_start(0)
    own_start(1)
    send_chunks(3)

    def first_norm(r, carry):
        at = pl.ds(pl.multiple_of(r * 32, 32), 32)
        n_one[at, :] = layer_norm(patches_ref[at, :], gain_ref[0:1, :], bias_ref[0:1, :])
        return carry

    lax.fori_loop(0, total_rows // 32, first_norm, 0)
    pump(0, 0)
    own_start(2)
    count_src[1] = count_finish(0)
    count_start(1)
    pump_from(0, 1)
    pump_from(1, 0)
    own_start(3)
    all_here(0)
    span = qkv.shape[2]
    for index in range(3):
        qkv[index] = jnp.dot(
            n_one[...], w_qkv[index], preferred_element_type=jnp.float32
        ).astype(jnp.bfloat16)
    pump(2, 0)
    send_chunks(4)

    def one_tile(tile, carry):
        at = pl.ds(pl.multiple_of(tile * PATCH, PATCH), PATCH)
        for low_col in range(0, span, VHD):
            cols = slice(low_col, low_col + VHD)
            scores = lax.dot_general(
                qkv[0, at, cols],
                qkv[1, at, cols],
                (((1,), (1,)), ((), ())),
                preferred_element_type=jnp.float32,
            ) * VHD ** (-0.5)
            grown = jnp.exp(scores - jnp.max(scores, axis=-1, keepdims=True))
            probs = (grown / jnp.sum(grown, axis=-1, keepdims=True)).astype(jnp.bfloat16)
            mixed[at, cols] = jnp.dot(
                probs, qkv[2, at, cols], preferred_element_type=jnp.float32
            ).astype(jnp.bfloat16)
        return carry

    lax.fori_loop(0, total_rows // PATCH, one_tile, 0)
    pump_from(2, 1)
    pump(3, 0)
    all_here(1)

    def projected(use, left, right):
        tile = 256

        def one(n, carry):
            at = pl.ds(pl.multiple_of(n * tile, tile), tile)
            partial[use, :, at] = lax.dot_general(
                left[...],
                right[at, :],
                (((1,), (1,)), ((), ())),
                preferred_element_type=jnp.float32,
            ).astype(jnp.bfloat16)
            return carry

        lax.fori_loop(0, width // tile, one, 0)

    def block_of(use, other, lane):
        start = (lax.rem(group + other, groups) * PAIR + lane) * rows
        return partial.at[use, pl.ds(pl.multiple_of(start, rows), rows)]

    def scatter(use):
        for other in list(range(1, groups)) + [0]:
            go(
                remote(
                    block_of(use, other, 1 - low),
                    pair_in.at[use, other],
                    pa_send.at[use, other],
                    pa_recv.at[use, other],
                    mp=partner,
                )
            )
        for other in range(1, groups):
            landed(pair_in.at[use, other], pa_recv.at[use, other])
            group_out[use, other - 1] = (
                block_of(use, other, low)[...].astype(jnp.float32)
                + pair_in[use, other].astype(jnp.float32)
            ).astype(jnp.bfloat16)
            go(
                remote(
                    group_out.at[use, other - 1],
                    group_in.at[use, other - 1],
                    pg_send.at[use, other],
                    pg_recv.at[use, other],
                    mp=lax.rem(group + other, groups) * PAIR + low,
                )
            )

    def scattered(use):
        landed(pair_in.at[use, 0], pa_recv.at[use, 0])
        value = block_of(use, 0, low)[...].astype(jnp.float32) + pair_in[use, 0].astype(
            jnp.float32
        )
        for other in range(1, groups):
            landed(group_in.at[use, other - 1], pg_recv.at[use, other])
            value = value + group_in[use, other - 1].astype(jnp.float32)
        return value

    def gather_start(use, view):
        mine = view(place)
        for step in range(1, groups):
            to = lax.rem(group + step, groups) * PAIR + low
            go(remote(mine, mine, ax_send.at[use, step], ax_recv.at[use, step], mp=to))
        go(remote(mine, mine, ad_send.at[use, 0], ad_recv.at[use, 0], mp=partner))

    def gather_finish(use, view):
        for step in range(1, groups):
            ref = view(lax.rem(group + groups - step, groups) * PAIR + low)
            landed(ref, ax_recv.at[use, step])
            go(remote(ref, ref, ad_send.at[use, step], ad_recv.at[use, step], mp=partner))
        for step in range(groups):
            landed(view(place), ad_recv.at[use, step])

    projected(0, mixed, w_out)
    scatter(0)
    send_chunks(5)
    pump(3, 1)
    own_start(4)
    resid[...] = (patches_ref[own_rows, :].astype(jnp.float32) + scattered(0)).astype(jnp.bfloat16)
    n_two[own_rows, :] = layer_norm(resid[...], gain_ref[1:2, :], bias_ref[1:2, :])

    def two_view(p):
        return n_two.at[pl.ds(pl.multiple_of(p * rows, rows), rows)]

    gather_start(0, two_view)
    count_src[2] = count_finish(1)
    count_start(2)
    pump_from(3, 2)
    gather_finish(0, two_view)
    send_chunks(7)
    forward_chunks(2)
    all_here(2)

    def hidden_tile(n, carry):
        at = pl.ds(pl.multiple_of(n * 256, 256), 256)
        made = jnp.dot(n_two[...], w_up[:, at], preferred_element_type=jnp.float32)
        inner[:, at] = (0.5 * made * (1.0 + lax.erf(made * 0.5**0.5))).astype(jnp.bfloat16)
        return carry

    lax.fori_loop(0, inner.shape[1] // 256, hidden_tile, 0)
    pump(4, 0)
    forward_chunks(4)
    all_here(3)
    projected(1, inner, w_down)
    scatter(1)
    send_chunks(10)

    item_rows = text_first.shape[1]

    def text_copy(half):
        return remote(
            text_ref.at[0, pl.ds(half * item_rows, item_rows)],
            text_first.at[place],
            tf_send.at[half],
            tf_recv.at[place],
            section=0,
            mp=section * PAIR + half,
        )

    early = (section < groups) & (place < AHEAD)
    for half in range(PAIR):
        here = (section == 0) & (place == half)

        @pl.when(early & here)
        def _():
            pltpu.make_async_copy(
                text_ref.at[0, pl.ds(half * item_rows, item_rows)],
                text_first.at[place],
                tf_recv.at[place],
            ).start()

        @pl.when(early & jnp.logical_not(here))
        def _():
            text_copy(half).start()

    states = (resid[...].astype(jnp.float32) + scattered(1)).astype(jnp.bfloat16)
    tokens = rows // 4
    row_id = lax.broadcasted_iota(jnp.int32, (rows, rows), 0)
    col_id = lax.broadcasted_iota(jnp.int32, (rows, rows), 1)
    spot, token = row_id // tokens, row_id % tokens
    across = GRID // 2
    source_row = (2 * (token // across) + spot // 2) * GRID + 2 * (token % across) + spot % 2
    picker = (source_row == col_id).astype(jnp.bfloat16)
    arranged = jnp.dot(picker, states, preferred_element_type=jnp.float32).astype(jnp.bfloat16)
    for spot_at in range(4):
        quads[spot_at] = arranged[spot_at * tokens : (spot_at + 1) * tokens, :]
    slice_width = pooled.shape[3]
    token_rows = pl.ds(pl.multiple_of(place * tokens, tokens), tokens)

    def slice_cols(at):
        return pl.ds(pl.multiple_of(at * slice_width, slice_width), slice_width)

    for step in range(1, replicas):
        to = lax.rem(replica + step, replicas)
        go(
            remote(
                quads.at[:, :, slice_cols(to)],
                pooled.at[replica, :, token_rows, :],
                pool_send.at[step],
                pool_recv.at[step],
                dp=to,
            )
        )
    pooled[replica, :, token_rows, :] = quads[:, :, slice_cols(replica)]
    for step in range(1, replicas):
        landed(pooled.at[replica, :, token_rows, :], pool_recv.at[step])

    def pool_view(p):
        return pooled.at[:, :, pl.ds(pl.multiple_of(p * tokens, tokens), tokens), :]

    gather_start(1, pool_view)
    pump(4, 1)
    gather_finish(1, pool_view)
    send_chunks(14)
    forward_chunks(7)
    pump_from(4, 2)
    all_here(4)
    all_tokens = pooled.shape[2]

    def image_tile(n, carry):
        at = pl.ds(pl.multiple_of(n * 256, 256), 256)
        value = None
        for spot_at in range(4):
            made = jnp.dot(
                pooled[:, spot_at].reshape(replicas * all_tokens, slice_width),
                w_proj[spot_at * slice_width : (spot_at + 1) * slice_width, at],
                preferred_element_type=jnp.float32,
            )
            value = made if value is None else value + made
        summed[:, :, at] = value.reshape(replicas, all_tokens, 256)
        return carry

    lax.fori_loop(0, summed.shape[2] // 256, image_tile, 0)
    for step in range(1, replicas):
        to = lax.rem(replica + step, replicas)
        far_out[step - 1] = summed[to].astype(jnp.bfloat16)
        go(
            remote(
                far_out.at[step - 1],
                far_in.at[step - 1],
                far_send.at[step],
                far_recv.at[step],
                dp=to,
            )
        )
    forward_chunks(8)
    value = summed[replica]
    for step in range(1, replicas):
        landed(far_in.at[step - 1], far_recv.at[step])
        value = value + far_in[step - 1].astype(jnp.float32)
    wide[group] = value.astype(jnp.bfloat16)
    for step in range(1, groups):
        to = lax.rem(group + step, groups) * PAIR + low
        go(remote(wide.at[group], wide.at[group], wide_send.at[step], wide_recv.at[step], mp=to))
    send_chunks(len(chunks))
    for step in range(1, groups):
        landed(wide.at[group], wide_recv.at[step])

    def image_copy(at):
        return remote(wide, image_own.at[at], im_send.at[0], im_recv.at[at], section=0)

    def pass_copy(at):
        source = wide if at == 0 else image_own.at[at]
        return remote(source, image_other.at[at], io_send.at[at], io_recv.at[at], mp=partner)

    for at in range(1, sections):

        @pl.when(section == at)
        def _():
            image_copy(at).start()

    @pl.when(section == 0)
    def _():
        pltpu.make_async_copy(wide, image_own.at[0], im_recv.at[0]).start()
        pass_copy(0).start()

    forward_chunks(11)

    order = [at for at in range(1, sections) if at in (1, sections - 1)]
    order = order + [at for at in range(1, sections) if at not in order]

    @pl.when(section == 0)
    def _():
        for at in order:
            landed(image_own.at[at], im_recv.at[at])
            pass_copy(at).start()

    forward_chunks(len(chunks))
    count_ref[...] = count_finish(2)

    for at in range(1, sections):

        @pl.when(section == at)
        def _():
            image_copy(at).wait_send()

    @pl.when(section == 0)
    def _():
        landed(wide, im_recv.at[0])
        for at in range(sections):
            landed(image_other.at[at], io_recv.at[at])
            pass_copy(at).wait_send()
        for item in range(AHEAD):
            landed(text_first.at[item], tf_recv.at[item])

    for half in range(PAIR):
        here = (section == 0) & (place == half)

        @pl.when(early & jnp.logical_not(here))
        def _():
            text_copy(half).wait_send()

    seg_here.wait()
    for step in range(1, sections):
        landed(seg_all.at[section], seg_recv.at[step])
    for u, (step, source, target) in enumerate(units):
        if u not in direct:
            landed(target, cy_recv.at[u])
    for w in range(len(weights)):
        ref = block_at(w, 0)
        for k in range(sections - 1):

            @pl.when((section >= k) & (section < sections - 1))
            def _():
                landed(ref, up_send.at[w, k])

            @pl.when((section + k <= sections - 1) & (section > 0))
            def _():
                landed(ref, dn_send.at[w, k])

        if weights[w][2]:
            for slot in range(sections * replicas):
                if slot % replicas:
                    landed(ref, y_send.at[w, slot])
    for copy in sent:
        copy.wait_send()


def run_vision(patches, vis_gain, vis_bias, loss_mask, segments, shards_of, text, w_query, w_kv, w_out):
    sections = lax.axis_size("section")
    replicas = lax.axis_size("dp")
    parts = lax.axis_size("mp")
    groups = parts // PAIR
    v_qkv, v_out, v_up, v_down, v_proj = shards_of
    total_rows, width = patches.shape
    rows = total_rows // parts
    tokens = rows // 4
    span = v_qkv.shape[2]
    units = (3 * IN_CHUNKS + OUT_BLOCKS - OUT_SHARED) * (groups - 1)
    bf, dma = jnp.bfloat16, pltpu.SemaphoreType.DMA
    vmem = pl.BlockSpec(memory_space=pltpu.VMEM)
    hbm = pl.BlockSpec(memory_space=pl.ANY)
    out_width = v_proj.shape[1]
    slice_width = v_proj.shape[0]
    shape = jax.ShapeDtypeStruct
    image = shape((sections, groups, tokens * parts, out_width), bf)
    levels = parts + replicas + sections
    pair_sem = dma((2, groups))
    ring_sem = dma((5, sections))
    return pl.pallas_call(
        functools.partial(vision_kernel, sections, replicas, parts),
        out_shape=[
            image,
            image,
            shape((sections,) + segments.shape[1:], jnp.int32),
            shape((8, loss_mask.shape[1]), jnp.int32),
            shape((AHEAD, text.shape[1] // PAIR, text.shape[2]), bf),
            shape((groups - 1,) + w_query.shape[1:], bf),
            shape((groups - 1,) + w_kv.shape[1:], bf),
            shape((groups - 1,) + w_out.shape[1:], bf),
        ],
        in_specs=[vmem] * 4 + [hbm] * 10,
        out_specs=[hbm] * 3 + [vmem] + [hbm] * 4,
        scratch_shapes=[
            pltpu.VMEM((3, width, span), bf),
            pltpu.VMEM((width, v_out.shape[0]), bf),
            pltpu.VMEM((width, v_up.shape[1]), bf),
            pltpu.VMEM((width, v_down.shape[0]), bf),
            pltpu.VMEM((sections * slice_width, out_width), bf),
            pltpu.VMEM((total_rows, width), bf),
            pltpu.VMEM((3, total_rows, span), bf),
            pltpu.VMEM((total_rows, span), bf),
            pltpu.VMEM((2, total_rows, width), bf),
            pltpu.VMEM((2, groups, rows, width), bf),
            pltpu.VMEM((2, groups, rows, width), bf),
            pltpu.VMEM((2, groups, rows, width), bf),
            pltpu.VMEM((rows, width), bf),
            pltpu.VMEM((total_rows, width), bf),
            pltpu.VMEM((total_rows, v_up.shape[1]), bf),
            pltpu.VMEM((4, tokens, width), bf),
            pltpu.VMEM((replicas, 4, tokens * parts, slice_width), bf),
            pltpu.VMEM((replicas, tokens * parts, out_width), jnp.float32),
            pltpu.VMEM((replicas, tokens * parts, out_width), bf),
            pltpu.VMEM((replicas, tokens * parts, out_width), bf),
            pltpu.VMEM((groups, tokens * parts, out_width), bf),
            pltpu.VMEM((levels, 8, loss_mask.shape[1]), jnp.int32),
            pltpu.VMEM((3, 8, loss_mask.shape[1]), jnp.int32),
            dma((5,)),
            dma((5, sections * replicas)),
            dma((5, sections * replicas)),
            ring_sem,
            ring_sem,
            ring_sem,
            ring_sem,
            pair_sem,
            pair_sem,
            pair_sem,
            pair_sem,
            pair_sem,
            pair_sem,
            pair_sem,
            pair_sem,
            dma((replicas,)),
            dma((replicas,)),
            dma((replicas,)),
            dma((replicas,)),
            dma((groups,)),
            dma((groups,)),
            dma((1,)),
            dma((sections,)),
            dma((sections,)),
            dma((sections,)),
            dma((units,)),
            dma((units,)),
            dma((units,)),
            dma((units,)),
            dma((PAIR,)),
            dma((PAIR,)),
            dma((sections,)),
            dma((sections,)),
            dma((levels,)),
            dma((levels,)),
        ],
        compiler_params=pltpu.CompilerParams(
            has_side_effects=True, vmem_limit_bytes=48 * 1024 * 1024
        ),
    )(
        patches,
        vis_gain,
        vis_bias,
        loss_mask,
        segments,
        v_qkv,
        v_out.T,
        v_up,
        v_down.T,
        v_proj,
        text,
        w_query,
        w_kv,
        w_out,
    )


def decoder_kernel(
    sections,
    parts,
    seqs,
    pick_ref,
    seg_row_ref,
    seg_col_ref,
    gain_ref,
    cos_ref,
    sin_ref,
    image_own_ref,
    image_other_ref,
    text_ref,
    first_ref,
    *refs,
):
    groups = parts // PAIR
    weight_refs = refs[: len(refs) - 27]
    (
        out_ref,
        w_in,
        w_out,
        arrived,
        normed,
        query,
        keyed,
        valued,
        bias,
        mixed,
        part,
        kept,
        give,
        take,
        done,
        home,
        w_sem,
        text_send,
        text_recv,
        n_send,
        n_recv,
        rs_send,
        rs_recv,
        hop_send,
        hop_recv,
        home_recv,
        turn,
    ) = refs[len(refs) - 27 :]
    section = lax.axis_index("section")
    place = lax.axis_index("mp")
    low = lax.rem(place, PAIR)
    group = place // PAIR
    partner = group * PAIR + (1 - low)
    items, own, width = arrived.shape
    chunk = PAIR * own
    piece = width // PIECES
    kv_width = keyed.shape[1]
    pair_heads = kv_width // HD
    heads = query.shape[0]
    each = heads // pair_heads
    last = sections - 1

    text_group = lax.rem(section, groups)
    text_item = (section // groups) * parts + place

    def text_copy(half):
        return pltpu.make_async_remote_copy(
            src_ref=text_ref.at[0, pl.ds(half * own, own)],
            dst_ref=arrived.at[text_item],
            send_sem=text_send.at[half],
            recv_sem=text_recv.at[text_item],
            device_id={"section": 0, "mp": text_group * PAIR + half},
            device_id_type=MESH,
        )

    @pl.when(section == 0)
    def _():
        for item in range(AHEAD):
            pltpu.make_async_copy(
                first_ref.at[item], arrived.at[item], text_recv.at[item]
            ).start()

    later = jnp.logical_not((section < groups) & (place < AHEAD))
    opens = ((section == groups) & (place == 0)) | ((section < groups) & (place == AHEAD))
    for half in range(PAIR):
        here = (section == 0) & (place == text_group * PAIR + half)

        @pl.when(later & here)
        def _():
            pltpu.make_async_copy(
                text_ref.at[0, pl.ds(half * own, own)],
                arrived.at[text_item],
                text_recv.at[text_item],
            ).start()

        @pl.when(later & (section == 0) & jnp.logical_not(here))
        def _():
            text_copy(half).start()

    in_loads, out_loads = weight_loads(weight_refs, w_in, w_out, groups)
    copies = [
        pltpu.make_async_copy(source, target, w_sem.at[at])
        for at, (source, target) in enumerate(in_loads + out_loads)
    ]
    for copy in copies:
        copy.start()
    keyed[...] = jnp.zeros_like(keyed)
    valued[...] = jnp.zeros_like(valued)
    first_count = len(in_loads)

    @pl.when(later & (section > 0))
    def _():
        @pl.when(jnp.logical_not(opens))
        def _():
            pl.semaphore_wait(turn, 1)

        for half in range(PAIR):
            text_copy(half).start()
        for half in range(PAIR):
            text_copy(half).wait_send()

        @pl.when(place < parts - 1)
        def _():
            pl.semaphore_signal(
                turn, 1, device_id={"mp": lax.rem(place + 1, parts)}, device_id_type=MESH
            )

        @pl.when((place == parts - 1) & (section + groups < sections))
        def _():
            pl.semaphore_signal(
                turn,
                1,
                device_id={"section": lax.rem(section + groups, sections), "mp": 0},
                device_id_type=MESH,
            )

    def one_item(item, carry):
        seq = item // parts
        at = lax.rem(item, parts)
        rows = pl.ds(pl.multiple_of(at * chunk, chunk), chunk)
        own_rows = pl.ds(pl.multiple_of(low * own, own), own)
        other_rows = pl.ds(pl.multiple_of((1 - low) * own, own), own)

        @pl.when(section == 0)
        def _():
            pltpu.make_async_copy(arrived.at[item], arrived.at[item], text_recv.at[item]).wait()
            cover = jnp.full((own, 1), pick_ref[item, 2], jnp.int32) > 0
            span = image_own_ref.shape[-1]
            for g in range(groups):
                for ref, lane in ((image_own_ref, low), (image_other_ref, 1 - low)):
                    cols = pl.ds(pl.multiple_of((g * PAIR + lane) * span, span), span)
                    arrived[item, :, cols] = jnp.where(
                        cover, ref[pick_ref[item, 0], g, pick_ref[item, 1]], arrived[item, :, cols]
                    )

        @pl.when(section > 0)
        def _():
            for t in range(PIECES):
                ref = arrived.at[item, :, pl.ds(t * piece, piece)]
                pltpu.make_async_copy(ref, ref, hop_recv.at[item, t]).wait()

        for r in range(0, own, 16):
            wide = arrived[item, r : r + 16, :].astype(jnp.float32)
            power = jnp.mean(wide * wide, axis=-1, keepdims=True)
            to = pl.ds(pl.multiple_of(low * own + r, 16), 16)
            normed[item, to, :] = (wide * lax.rsqrt(power + EPS) * gain_ref[...]).astype(
                jnp.bfloat16
            )
        n_copy = pltpu.make_async_remote_copy(
            src_ref=normed.at[item, own_rows],
            dst_ref=normed.at[item, own_rows],
            send_sem=n_send.at[item],
            recv_sem=n_recv.at[item],
            device_id={"mp": partner},
            device_id_type=MESH,
        )
        n_copy.start()
        allowed = (seg_col_ref[seq, rows, :] == seg_row_ref[seq]) & (
            lax.broadcasted_iota(jnp.int32, bias.shape, 1)
            <= lax.broadcasted_iota(jnp.int32, bias.shape, 0) + at * chunk
        )
        bias[...] = jnp.where(allowed, 0.0, BLOCKED)

        @pl.when(item == 0)
        def _():
            for copy in copies[:first_count]:
                copy.wait()

        n_copy.wait_recv()

        cosine, sinus = cos_ref[rows, :], sin_ref[rows, :]

        def turned(col):
            made = jnp.dot(
                normed[item],
                w_in[:, pl.ds(pl.multiple_of(col, kv_width), kv_width)],
                preferred_element_type=jnp.float32,
            )
            outs = []
            for h in range(pair_heads):
                head = made[:, h * HD : (h + 1) * HD]
                outs.append(
                    (head * cosine + pltpu.roll(head, HD // 2, 1) * sinus).astype(jnp.bfloat16)
                )
            return outs

        def query_tile(tile, c):
            for h, value in enumerate(turned(tile * kv_width)):
                query[tile * pair_heads + h] = value
            return c

        lax.fori_loop(0, heads // pair_heads, query_tile, 0)
        for h, value in enumerate(turned(heads * HD)):
            keyed[rows, h * HD : (h + 1) * HD] = value
        valued[rows, :] = jnp.dot(
            normed[item],
            w_in[:, heads * HD + kv_width :],
            preferred_element_type=jnp.float32,
        ).astype(jnp.bfloat16)

        for h in range(heads):
            kv = slice((h // each) * HD, (h // each + 1) * HD)
            scores = (
                lax.dot_general(
                    query[h],
                    keyed[:, kv],
                    (((1,), (1,)), ((), ())),
                    preferred_element_type=jnp.float32,
                )
                * HD ** (-0.5)
                + bias[...]
            )
            high = jnp.max(scores, axis=-1, keepdims=True)
            grown = jnp.exp(scores - high)
            probs = (grown / jnp.sum(grown, axis=-1, keepdims=True)).astype(jnp.bfloat16)
            mixed[:, h * HD : (h + 1) * HD] = jnp.dot(
                probs, valued[:, kv], preferred_element_type=jnp.float32
            ).astype(jnp.bfloat16)

        @pl.when(item == 0)
        def _():
            for copy in copies[first_count:]:
                copy.wait()

        def give_copy(t):
            return pltpu.make_async_remote_copy(
                src_ref=give.at[item, :, pl.ds(t * piece, piece)],
                dst_ref=take.at[item, :, pl.ds(t * piece, piece)],
                send_sem=rs_send.at[item, t],
                recv_sem=rs_recv.at[item, t],
                device_id={"mp": partner},
                device_id_type=MESH,
            )

        for t in range(PIECES):
            cols = slice(t * piece, (t + 1) * piece)
            part[...] = jnp.dot(mixed[...], w_out[:, cols], preferred_element_type=jnp.float32)
            give[item, :, cols] = part[other_rows, :].astype(jnp.bfloat16)
            give_copy(t).start()
            kept[:, cols] = part[own_rows, :] + arrived[item, :, cols].astype(jnp.float32)

        goal = seq * groups + group
        stays = (section == last) & (goal == last) & (at == place)
        for t in range(PIECES):
            cols = slice(t * piece, (t + 1) * piece)
            give_copy(t).wait_recv()
            done[item, :, cols] = (
                kept[:, cols] + take[item, :, cols].astype(jnp.float32)
            ).astype(jnp.bfloat16)

            @pl.when(section < last)
            def _():
                hop_copy(item, t).start()

            @pl.when((section == last) & jnp.logical_not(stays))
            def _():
                home_copy(item, t).start()

            @pl.when(stays)
            def _():
                home[own_rows, cols] = done[item, :, cols]

        return carry

    def hop_copy(item, t):
        return pltpu.make_async_remote_copy(
            src_ref=done.at[item, :, pl.ds(t * piece, piece)],
            dst_ref=arrived.at[item, :, pl.ds(t * piece, piece)],
            send_sem=hop_send.at[item, t],
            recv_sem=hop_recv.at[item, t],
            device_id={"section": lax.rem(section + 1, sections)},
            device_id_type=MESH,
        )

    def home_copy(item, t):
        return pltpu.make_async_remote_copy(
            src_ref=done.at[item, :, pl.ds(t * piece, piece)],
            dst_ref=home.at[pl.ds(pl.multiple_of(low * own, own), own), pl.ds(t * piece, piece)],
            send_sem=hop_send.at[item, t],
            recv_sem=home_recv.at[low, t],
            device_id={"section": (item // parts) * groups + group, "mp": lax.rem(item, parts)},
            device_id_type=MESH,
        )

    lax.fori_loop(0, items, one_item, 0)

    for half in range(PAIR):
        here = (section == 0) & (place == text_group * PAIR + half)

        @pl.when(later & (section == 0) & jnp.logical_not(here))
        def _():
            text_copy(half).wait_send()

    def drain(item, carry):
        n_ref = normed.at[item, pl.ds(0, own)]
        pltpu.make_async_copy(n_ref, n_ref, n_send.at[item]).wait()
        goal = (item // parts) * groups + group
        stays = (section == last) & (goal == last) & (lax.rem(item, parts) == place)
        for t in range(PIECES):
            ref = give.at[item, :, pl.ds(t * piece, piece)]
            pltpu.make_async_copy(ref, ref, rs_send.at[item, t]).wait()

            @pl.when(jnp.logical_not(stays))
            def _():
                ref = done.at[item, :, pl.ds(t * piece, piece)]
                pltpu.make_async_copy(ref, ref, hop_send.at[item, t]).wait()

        return carry

    lax.fori_loop(0, items, drain, 0)
    for half in range(PAIR):
        sender = lax.rem(section, groups) * PAIR + half

        @pl.when(jnp.logical_not((section == last) & (place == sender)))
        def _():
            for t in range(PIECES):
                ref = home.at[pl.ds(half * own, own), pl.ds(t * piece, piece)]
                pltpu.make_async_copy(ref, ref, home_recv.at[half, t]).wait()

    out_ref[0] = home[...]


def weight_loads(refs, w_in, w_out, groups):
    query_ref, kv_ref, out_ref = refs[:3]
    query_span, kv_span, out_span = query_ref.shape[2], kv_ref.shape[3], out_ref.shape[1]
    keys_at, values_at = query_span * groups, (query_span + kv_span) * groups
    in_loads = [
        (query_ref.at[0], w_in.at[:, pl.ds(0, query_span)]),
        (kv_ref.at[0, 0], w_in.at[:, pl.ds(keys_at, kv_span)]),
        (kv_ref.at[0, 1], w_in.at[:, pl.ds(values_at, kv_span)]),
    ]
    out_loads = [(out_ref.at[0], w_out.at[pl.ds(0, out_span)])]
    other_q, other_kv, other_o = refs[3:]
    for other in range(1, groups):
        cols = pl.ds(other * query_span, query_span)
        in_loads.append((other_q.at[other - 1], w_in.at[:, cols]))
        for index, at in ((0, keys_at), (1, values_at)):
            cols = pl.ds(at + other * kv_span, kv_span)
            in_loads.append((other_kv.at[other - 1, index], w_in.at[:, cols]))
        out_loads.append((other_o.at[other - 1], w_out.at[pl.ds(other * out_span, out_span)]))
    return in_loads, out_loads


def run_decoder(text, first, image_own, image_other, pick, segs, gain, cosine, sinus, weights, sections, parts):
    seqs, length = segs.shape
    width = text.shape[2]
    chunk = text.shape[1]
    own = chunk // PAIR
    items = seqs * parts
    groups = parts // PAIR
    query_width, kv_width = weights[0].shape[2] * groups, weights[1].shape[3] * groups
    joined = query_width + 2 * kv_width
    loads = 4 * groups
    vmem = pl.BlockSpec(memory_space=pltpu.VMEM)
    hbm = pl.BlockSpec(memory_space=pl.ANY)
    smem = pl.BlockSpec(memory_space=pltpu.SMEM)
    dma = pltpu.SemaphoreType.DMA
    bf = jnp.bfloat16
    return pl.pallas_call(
        functools.partial(decoder_kernel, sections, parts, seqs),
        out_shape=jax.ShapeDtypeStruct(text.shape, text.dtype),
        in_specs=[smem] + [vmem] * 7 + [hbm] * (2 + len(weights)),
        out_specs=vmem,
        scratch_shapes=[
            pltpu.VMEM((width, joined), bf),
            pltpu.VMEM((query_width, width), bf),
            pltpu.VMEM((items, own, width), bf),
            pltpu.VMEM((items, chunk, width), bf),
            pltpu.VMEM((query_width // HD, chunk, HD), bf),
            pltpu.VMEM((length, kv_width), bf),
            pltpu.VMEM((length, kv_width), bf),
            pltpu.VMEM((chunk, length), jnp.float32),
            pltpu.VMEM((chunk, query_width), bf),
            pltpu.VMEM((chunk, width // PIECES), jnp.float32),
            pltpu.VMEM((own, width), jnp.float32),
            pltpu.VMEM((items, own, width), bf),
            pltpu.VMEM((items, own, width), bf),
            pltpu.VMEM((items, own, width), bf),
            pltpu.VMEM((chunk, width), bf),
            dma((loads,)),
            dma((PAIR,)),
            dma((items,)),
            dma((items,)),
            dma((items,)),
            dma((items, PIECES)),
            dma((items, PIECES)),
            dma((items, PIECES)),
            dma((items, PIECES)),
            dma((PAIR, PIECES)),
            pltpu.SemaphoreType.REGULAR,
        ],
        compiler_params=pltpu.CompilerParams(
            has_side_effects=True, vmem_limit_bytes=63 * 1024 * 1024
        ),
        cost_estimate=pl.CostEstimate(
            flops=2 * items * chunk * width * (joined + query_width),
            bytes_accessed=2 * width * (joined + query_width),
            transcendentals=0,
        ),
    )(
        pick,
        segs[:, None, :],
        segs[:, :, None],
        gain,
        cosine,
        sinus,
        image_own,
        image_other,
        text,
        first,
        *weights,
    )


def shards(
    text,
    patches,
    segments,
    loss_mask,
    tile_batch,
    tile_offset,
    attn_gain,
    w_query,
    w_kv,
    w_out,
    vis_gain,
    vis_bias,
    v_qkv,
    v_out,
    v_up,
    v_down,
    v_proj,
):
    sections = lax.axis_size("section")
    replicas = lax.axis_size("dp")
    parts = lax.axis_size("mp")
    groups = parts // PAIR
    part_at = lax.axis_index("mp")
    low_at = part_at % PAIR
    group_at = part_at // PAIR
    length = segments.shape[2]

    image_own, image_other, seg_all, counts, first, other_q, other_kv, other_o = run_vision(
        patches,
        vis_gain,
        vis_bias,
        loss_mask,
        segments,
        (v_qkv, v_out, v_up, v_down, v_proj),
        text,
        w_query,
        w_kv,
        w_out,
    )
    seqs = sections // groups
    seg_mine = jnp.take(seg_all.reshape(seqs, groups, length), group_at, axis=1)
    scaling = float(sections * replicas * length)
    token_weight = loss_mask.astype(jnp.float32) * scaling / jnp.sum(counts).astype(jnp.float32)
    tiles_here = image_own.shape[2] // POOL
    blocks = (sections, groups, tiles_here, POOL, image_own.shape[3])

    batch_all = tile_batch[0]
    offset_all = tile_offset[0]
    items = seqs * parts
    item_ids = jnp.arange(items, dtype=jnp.int32)
    item_batch = (item_ids // parts) * groups + group_at
    chunk = text.shape[1]
    item_place = (item_ids % parts) * chunk + low_at * (chunk // PAIR)
    hit = (batch_all[None, :] == item_batch[:, None]) & (
        offset_all[None, :] == item_place[:, None]
    )
    tile_at = jnp.sum(hit * jnp.arange(batch_all.shape[0], dtype=jnp.int32)[None, :], axis=1)
    pick = jnp.stack(
        [tile_at // tiles_here, tile_at % tiles_here, jnp.any(hit, axis=1).astype(jnp.int32)],
        axis=1,
    ).astype(jnp.int32)

    positions = jnp.arange(length, dtype=jnp.int32)
    freqs = ROPE_BASE ** (-2.0 * jnp.arange(HD // 2, dtype=jnp.float32) / HD)
    angles = positions.astype(jnp.float32)[:, None] * freqs[None, :]
    cosine, sinus = jnp.cos(angles), jnp.sin(angles)
    cos_full = jnp.concatenate([cosine, cosine], axis=1)
    sin_full = jnp.concatenate([-sinus, sinus], axis=1)

    hidden = run_decoder(
        text,
        first,
        image_own.reshape(blocks),
        image_other.reshape(blocks),
        pick,
        seg_mine,
        attn_gain,
        cos_full,
        sin_full,
        [w_query, w_kv, w_out, other_q, other_kv, other_o],
        sections,
        parts,
    )
    return (hidden, token_weight)


def solution(mesh):
    in_specs = (
        P("section", ("dp", "mp"), None),
        P(("section", "dp"), None),
        P("section", "dp", None),
        P("section", ("dp", "mp")),
        P("dp", None),
        P("dp", None),
        P("section", None),
        P("section", None, "mp"),
        P("section", None, None, "mp"),
        P("section", "mp", None),
        P(),
        P(),
        P(None, ("section", "dp"), "mp"),
        P("mp", ("section", "dp")),
        P(("section", "dp"), "mp"),
        P("mp", ("section", "dp")),
        P(("section", "dp"), "mp"),
    )
    out_specs = (P("section", ("dp", "mp"), None), P("section", ("dp", "mp")))
    return jax.shard_map(shards, mesh=mesh, in_specs=in_specs, out_specs=out_specs, check_vma=False)
```

```python
import functools

import jax
import jax.numpy as jnp
from jax import lax
from jax.experimental import pallas as pl
from jax.experimental.pallas import tpu as pltpu
from jax.sharding import PartitionSpec as P

HD = 128
VHD = 64
GRID = 16
PATCH = 256
POOL = 64


EPS = 1e-05
ROPE_BASE = 500000.0
BLOCKED = -1e30
PAIR = 2
PIECES = 4
MESH = pl.DeviceIdType.MESH


def layer_norm(values, gain, bias):
    wide = values.astype(jnp.float32)
    center = wide - jnp.mean(wide, axis=-1, keepdims=True)
    spread = jnp.mean(center * center, axis=-1, keepdims=True)
    return (center * lax.rsqrt(spread + EPS) * gain + bias).astype(jnp.bfloat16)


def remote(source, target, send_sem, recv_sem, **device):
    return pltpu.make_async_remote_copy(
        src_ref=source,
        dst_ref=target,
        send_sem=send_sem,
        recv_sem=recv_sem,
        device_id=device,
        device_id_type=MESH,
    )


def landed(ref, sem):
    pltpu.make_async_copy(ref, ref, sem).wait()


def block_rows(ref, start, count):
    rows = pl.ds(pl.multiple_of(start, 16), count)
    return ref.at[:, rows] if len(ref.shape) == 3 else ref.at[rows]


IN_CHUNKS = 8
OUT_BLOCKS = 16
OUT_SHARED = 6
AHEAD = 1
FIRST, AFTER, NEVER = 0, 1, 2


def vision_kernel(
    sections,
    replicas,
    parts,
    patches_ref,
    gain_ref,
    bias_ref,
    loss_ref,
    seg_ref,
    qkv_src,
    out_src,
    up_src,
    down_src,
    proj_src,
    text_ref,
    wq_ref,
    wkv_ref,
    wo_ref,
    image,
    seg_all,
    count_ref,
    text_first,
    other_q,
    other_kv,
    other_o,
    w_qkv,
    w_out,
    w_up,
    w_down,
    w_proj,
    n_one,
    qkv,
    mixed,
    partial,
    pair_in,
    group_out,
    group_in,
    resid,
    n_two,
    inner,
    quads,
    pooled,
    summed,
    far_out,
    far_in,
    wide,
    counts,
    count_src,
    local_sem,
    y_send,
    y_recv,
    up_send,
    up_recv,
    dn_send,
    dn_recv,
    pa_send,
    pa_recv,
    pg_send,
    pg_recv,
    ax_send,
    ax_recv,
    ad_send,
    ad_recv,
    pool_send,
    pool_recv,
    far_send,
    far_recv,
    im_send,
    im_recv,
    gx_send,
    gx_recv,
    gd_send,
    gd_recv,
    cx_send,
    cx_recv,
    cy_send,
    cy_recv,
    tf_send,
    tf_recv,
    seg_send,
    seg_recv,
    cnt_send,
    cnt_recv,
):
    groups = parts // PAIR
    section = lax.axis_index("section")
    replica = lax.axis_index("dp")
    place = lax.axis_index("mp")
    low = lax.rem(place, PAIR)
    group = place // PAIR
    partner = group * PAIR + (1 - low)
    after = lax.rem(section + 1, sections)
    before = lax.rem(section + sections - 1, sections)
    even = lax.rem(replica, 2)
    mate = replica + 1 - 2 * even
    total_rows, width = patches_ref.shape
    rows = total_rows // parts
    own_rows = pl.ds(pl.multiple_of(place * rows, rows), rows)
    sent = []

    def go(copy):
        copy.start()
        sent.append(copy)

    axes = (("mp", place, parts), ("dp", replica, replicas), ("section", section, sections))

    def count_start(level):
        axis, at, size = axes[level]
        slot = sum(axes[i][2] for i in range(level))
        counts[slot + at] = count_src[level]
        for step in range(1, size):
            go(
                remote(
                    count_src.at[level],
                    counts.at[slot + at],
                    cnt_send.at[slot + step],
                    cnt_recv.at[slot + step],
                    **{axis: lax.rem(at + step, size)},
                )
            )

    def count_finish(level):
        size = axes[level][2]
        slot = sum(axes[i][2] for i in range(level))
        for step in range(1, size):
            landed(count_src.at[level], cnt_recv.at[slot + step])
        value = counts[slot]
        for at in range(1, size):
            value = value + counts[slot + at]
        return value

    first_row = lax.broadcasted_iota(jnp.int32, count_ref.shape, 0) == 0
    count_src[0] = jnp.where(first_row, jnp.broadcast_to(loss_ref[...], count_ref.shape), 0)
    count_start(0)

    for step in range(1, sections):
        go(
            remote(
                seg_ref.at[0],
                seg_all.at[section],
                seg_send.at[step],
                seg_recv.at[step],
                section=lax.rem(section + step, sections),
            )
        )
    seg_here = pltpu.make_async_copy(seg_ref.at[0], seg_all.at[section], seg_recv.at[0])
    seg_here.start()

    weights = [
        (qkv_src, w_qkv, AFTER),
        (out_src, w_out, AFTER),
        (up_src, w_up, AFTER),
        (down_src, w_down, AFTER),
        (proj_src, w_proj, NEVER),
    ]

    def block_at(w, block):
        source, buffer, kind = weights[w]
        count = source.shape[-2]
        if kind == FIRST:
            return block_rows(buffer, block * replicas * count, replicas * count)
        if kind == AFTER:
            return block_rows(buffer, (block * replicas + replica) * count, count)
        return block_rows(buffer, block * count, count)

    def up_copy(w, k, source, target):
        return remote(source, target, up_send.at[w, k], up_recv.at[w, k], section=after)

    def down_copy(w, k, source, target):
        return remote(source, target, dn_send.at[w, k], dn_recv.at[w, k], section=before)

    def share(w, block, source):
        if weights[w][2] == AFTER:
            for step in range(1, replicas):
                slot = block * replicas + step
                remote(
                    source,
                    block_at(w, block),
                    y_send.at[w, slot],
                    y_recv.at[w, slot],
                    dp=lax.rem(replica + step, replicas),
                ).start()

    def first_share(w):
        source, buffer, kind = weights[w]
        count = source.shape[-2]
        target = block_rows(buffer, (section * replicas + replica) * count, count)
        pltpu.make_async_copy(source, target, local_sem.at[w]).start()
        for step in range(1, replicas):
            go(
                remote(
                    source,
                    target,
                    y_send.at[w, step],
                    y_recv.at[w, step],
                    dp=lax.rem(replica + step, replicas),
                )
            )

    def own_start(w):
        source, buffer, kind = weights[w]
        target = block_at(w, section)
        if kind == FIRST:
            own = block_rows(buffer, 0, source.shape[-2])
            landed(own, local_sem.at[w])
            for step in range(1, replicas):
                landed(own, y_recv.at[w, step])
            source = target
        else:
            pltpu.make_async_copy(source, target, local_sem.at[w]).start()

        @pl.when(section < sections - 1)
        def _():
            up_copy(w, 0, source, target).start()

        @pl.when(section > 0)
        def _():
            down_copy(w, 0, source, target).start()

        share(w, section, source)

    def pump(w, k):
        @pl.when(section >= k + 1)
        def _():
            block = section - 1 - k
            ref = block_at(w, block)
            landed(ref, up_recv.at[w, k])

            @pl.when(section < sections - 1)
            def _():
                up_copy(w, k + 1, ref, ref).start()

            share(w, block, ref)

        @pl.when(section + k + 1 <= sections - 1)
        def _():
            block = section + 1 + k
            ref = block_at(w, block)
            landed(ref, dn_recv.at[w, k])

            @pl.when(section > 0)
            def _():
                down_copy(w, k + 1, ref, ref).start()

            share(w, block, ref)

    def pump_from(w, k):
        for at in range(k, sections - 1):
            pump(w, at)

    def all_here(w):
        if weights[w][2] != FIRST:
            landed(block_at(w, 0), local_sem.at[w])
        if weights[w][2] == AFTER:
            for slot in range(sections * replicas):
                if slot % replicas:
                    landed(block_at(w, 0), y_recv.at[w, slot])

    units, chunks, direct = [], [], []
    for step in range(1, groups):
        depth = wq_ref.shape[1] // 2 // IN_CHUNKS
        for c in range(IN_CHUNKS):
            at = pl.ds(pl.multiple_of((even * IN_CHUNKS + c) * depth, depth), depth)
            chunks.append([len(units) + i for i in range(3)])
            units.append((step, wq_ref.at[0, at], other_q.at[step - 1, at]))
            units.append((step, wkv_ref.at[0, 0, at], other_kv.at[step - 1, 0, at]))
            units.append((step, wkv_ref.at[0, 1, at], other_kv.at[step - 1, 1, at]))
    for step in range(1, groups):
        depth = wo_ref.shape[1] // OUT_BLOCKS
        for c in range(OUT_BLOCKS - OUT_SHARED):
            block = even * OUT_SHARED + c if c < OUT_SHARED else OUT_SHARED + c
            at = pl.ds(pl.multiple_of(block * depth, depth), depth)
            chunks.append([len(units)])
            if c >= OUT_SHARED:
                direct.append(len(units))
            units.append((step, wo_ref.at[0, at], other_o.at[step - 1, at]))
    progress = {"x": 0, "y": 0}

    def send_chunks(upto):
        while progress["x"] < min(upto, len(chunks)):
            for u in chunks[progress["x"]]:
                step, source, target = units[u]
                to = lax.rem(group + step, groups) * PAIR + low
                go(remote(source, target, cx_send.at[u], cx_recv.at[u], mp=to))
            progress["x"] += 1

    def forward_chunks(upto):
        while progress["y"] < min(upto, len(chunks)):
            for u in chunks[progress["y"]]:
                step, source, target = units[u]
                landed(target, cx_recv.at[u])
                if u in direct:
                    continue
                go(remote(target, target, cy_send.at[u], cy_recv.at[u], dp=mate))
            progress["y"] += 1

    own_start(0)
    own_start(1)
    send_chunks(3)

    def first_norm(r, carry):
        at = pl.ds(pl.multiple_of(r * 32, 32), 32)
        n_one[at, :] = layer_norm(patches_ref[at, :], gain_ref[0:1, :], bias_ref[0:1, :])
        return carry

    lax.fori_loop(0, total_rows // 32, first_norm, 0)
    pump(0, 0)
    own_start(2)
    count_src[1] = count_finish(0)
    count_start(1)
    pump_from(0, 1)
    pump_from(1, 0)
    own_start(3)
    all_here(0)
    span = qkv.shape[2]
    for index in range(3):
        qkv[index] = jnp.dot(
            n_one[...], w_qkv[index], preferred_element_type=jnp.float32
        ).astype(jnp.bfloat16)
    pump(2, 0)
    send_chunks(4)

    def one_tile(tile, carry):
        at = pl.ds(pl.multiple_of(tile * PATCH, PATCH), PATCH)
        for low_col in range(0, span, VHD):
            cols = slice(low_col, low_col + VHD)
            scores = lax.dot_general(
                qkv[0, at, cols],
                qkv[1, at, cols],
                (((1,), (1,)), ((), ())),
                preferred_element_type=jnp.float32,
            ) * VHD ** (-0.5)
            grown = jnp.exp(scores - jnp.max(scores, axis=-1, keepdims=True))
            probs = (grown / jnp.sum(grown, axis=-1, keepdims=True)).astype(jnp.bfloat16)
            mixed[at, cols] = jnp.dot(
                probs, qkv[2, at, cols], preferred_element_type=jnp.float32
            ).astype(jnp.bfloat16)
        return carry

    lax.fori_loop(0, total_rows // PATCH, one_tile, 0)
    pump_from(2, 1)
    pump(3, 0)
    all_here(1)

    def projected(use, left, right):
        tile = 256

        def one(n, carry):
            at = pl.ds(pl.multiple_of(n * tile, tile), tile)
            partial[use, :, at] = lax.dot_general(
                left[...],
                right[at, :],
                (((1,), (1,)), ((), ())),
                preferred_element_type=jnp.float32,
            ).astype(jnp.bfloat16)
            return carry

        lax.fori_loop(0, width // tile, one, 0)

    def block_of(use, other, lane):
        start = (lax.rem(group + other, groups) * PAIR + lane) * rows
        return partial.at[use, pl.ds(pl.multiple_of(start, rows), rows)]

    def scatter(use):
        for other in list(range(1, groups)) + [0]:
            go(
                remote(
                    block_of(use, other, 1 - low),
                    pair_in.at[use, other],
                    pa_send.at[use, other],
                    pa_recv.at[use, other],
                    mp=partner,
                )
            )
        for other in range(1, groups):
            landed(pair_in.at[use, other], pa_recv.at[use, other])
            group_out[use, other - 1] = (
                block_of(use, other, low)[...].astype(jnp.float32)
                + pair_in[use, other].astype(jnp.float32)
            ).astype(jnp.bfloat16)
            go(
                remote(
                    group_out.at[use, other - 1],
                    group_in.at[use, other - 1],
                    pg_send.at[use, other],
                    pg_recv.at[use, other],
                    mp=lax.rem(group + other, groups) * PAIR + low,
                )
            )

    def scattered(use):
        landed(pair_in.at[use, 0], pa_recv.at[use, 0])
        value = block_of(use, 0, low)[...].astype(jnp.float32) + pair_in[use, 0].astype(
            jnp.float32
        )
        for other in range(1, groups):
            landed(group_in.at[use, other - 1], pg_recv.at[use, other])
            value = value + group_in[use, other - 1].astype(jnp.float32)
        return value

    def gather_start(use, view):
        mine = view(place)
        for step in range(1, groups):
            to = lax.rem(group + step, groups) * PAIR + low
            go(remote(mine, mine, ax_send.at[use, step], ax_recv.at[use, step], mp=to))
        go(remote(mine, mine, ad_send.at[use, 0], ad_recv.at[use, 0], mp=partner))

    def gather_finish(use, view):
        for step in range(1, groups):
            ref = view(lax.rem(group + groups - step, groups) * PAIR + low)
            landed(ref, ax_recv.at[use, step])
            go(remote(ref, ref, ad_send.at[use, step], ad_recv.at[use, step], mp=partner))
        for step in range(groups):
            landed(view(place), ad_recv.at[use, step])

    projected(0, mixed, w_out)
    scatter(0)
    send_chunks(5)
    pump(3, 1)
    own_start(4)
    resid[...] = (patches_ref[own_rows, :].astype(jnp.float32) + scattered(0)).astype(jnp.bfloat16)
    n_two[own_rows, :] = layer_norm(resid[...], gain_ref[1:2, :], bias_ref[1:2, :])

    def two_view(p):
        return n_two.at[pl.ds(pl.multiple_of(p * rows, rows), rows)]

    gather_start(0, two_view)
    count_src[2] = count_finish(1)
    count_start(2)
    pump_from(3, 2)
    gather_finish(0, two_view)
    send_chunks(7)
    forward_chunks(2)
    all_here(2)

    def hidden_tile(n, carry):
        at = pl.ds(pl.multiple_of(n * 256, 256), 256)
        made = jnp.dot(n_two[...], w_up[:, at], preferred_element_type=jnp.float32)
        inner[:, at] = (0.5 * made * (1.0 + lax.erf(made * 0.5**0.5))).astype(jnp.bfloat16)
        return carry

    lax.fori_loop(0, inner.shape[1] // 256, hidden_tile, 0)
    pump(4, 0)
    forward_chunks(4)
    all_here(3)
    projected(1, inner, w_down)
    scatter(1)
    send_chunks(10)

    states = (resid[...].astype(jnp.float32) + scattered(1)).astype(jnp.bfloat16)
    tokens = rows // 4
    row_id = lax.broadcasted_iota(jnp.int32, (rows, rows), 0)
    col_id = lax.broadcasted_iota(jnp.int32, (rows, rows), 1)
    spot, token = row_id // tokens, row_id % tokens
    across = GRID // 2
    source_row = (2 * (token // across) + spot // 2) * GRID + 2 * (token % across) + spot % 2
    picker = (source_row == col_id).astype(jnp.bfloat16)
    arranged = jnp.dot(picker, states, preferred_element_type=jnp.float32).astype(jnp.bfloat16)
    for spot_at in range(4):
        quads[spot_at] = arranged[spot_at * tokens : (spot_at + 1) * tokens, :]
    slice_width = pooled.shape[3]
    token_rows = pl.ds(pl.multiple_of(place * tokens, tokens), tokens)

    def slice_cols(at):
        return pl.ds(pl.multiple_of(at * slice_width, slice_width), slice_width)

    for step in range(1, replicas):
        to = lax.rem(replica + step, replicas)
        go(
            remote(
                quads.at[:, :, slice_cols(to)],
                pooled.at[replica, :, token_rows, :],
                pool_send.at[step],
                pool_recv.at[step],
                dp=to,
            )
        )
    pooled[replica, :, token_rows, :] = quads[:, :, slice_cols(replica)]
    for step in range(1, replicas):
        landed(pooled.at[replica, :, token_rows, :], pool_recv.at[step])

    def pool_view(p):
        return pooled.at[:, :, pl.ds(pl.multiple_of(p * tokens, tokens), tokens), :]

    gather_start(1, pool_view)
    pump(4, 1)
    item_rows = text_first.shape[1]

    def text_copy(half):
        return remote(
            text_ref.at[0, pl.ds(half * item_rows, item_rows)],
            text_first.at[place],
            tf_send.at[half],
            tf_recv.at[place],
            section=0,
            mp=section * PAIR + half,
        )

    early = ((section == 0) & (place < AHEAD)) | ((section > 0) & (section < groups))
    for half in range(PAIR):
        here = (section == 0) & (place == half)

        @pl.when(early & here)
        def _():
            pltpu.make_async_copy(
                text_ref.at[0, pl.ds(half * item_rows, item_rows)],
                text_first.at[place],
                tf_recv.at[place],
            ).start()

        @pl.when(early & jnp.logical_not(here))
        def _():
            text_copy(half).start()

    gather_finish(1, pool_view)
    send_chunks(14)
    forward_chunks(7)
    pump_from(4, 2)
    all_here(4)
    all_tokens = pooled.shape[2]

    def image_tile(n, carry):
        at = pl.ds(pl.multiple_of(n * 256, 256), 256)
        value = None
        for spot_at in range(4):
            made = jnp.dot(
                pooled[:, spot_at].reshape(replicas * all_tokens, slice_width),
                w_proj[spot_at * slice_width : (spot_at + 1) * slice_width, at],
                preferred_element_type=jnp.float32,
            )
            value = made if value is None else value + made
        summed[:, :, at] = value.reshape(replicas, all_tokens, 256)
        return carry

    lax.fori_loop(0, summed.shape[2] // 256, image_tile, 0)
    for step in range(1, replicas):
        to = lax.rem(replica + step, replicas)
        far_out[step - 1] = summed[to].astype(jnp.bfloat16)
        go(
            remote(
                far_out.at[step - 1],
                far_in.at[step - 1],
                far_send.at[step],
                far_recv.at[step],
                dp=to,
            )
        )
    forward_chunks(8)
    value = summed[replica]
    for step in range(1, replicas):
        landed(far_in.at[step - 1], far_recv.at[step])
        value = value + far_in[step - 1].astype(jnp.float32)
    wide[...] = value.astype(jnp.bfloat16)

    def image_copy(at):
        return remote(wide, image.at[at, place], im_send.at[0], im_recv.at[at], section=0)

    def across_copy(at, step):
        to = lax.rem(group + step, groups) * PAIR + low
        source = wide if at == 0 else image.at[at, place]
        return remote(
            source, image.at[at, place], gx_send.at[at, step], gx_recv.at[at, step], mp=to
        )

    def beside_copy(at, step):
        from_place = lax.rem(group + groups - step, groups) * PAIR + low
        source = wide if at == 0 and step == 0 else image.at[at, from_place]
        return remote(
            source,
            image.at[at, from_place],
            gd_send.at[at, step],
            gd_recv.at[at, step],
            mp=partner,
        )

    for at in range(1, sections):

        @pl.when(section == at)
        def _():
            image_copy(at).start()

    @pl.when(section == 0)
    def _():
        pltpu.make_async_copy(wide, image.at[0, place], im_recv.at[0]).start()
        for at in range(sections):
            if at > 0:
                landed(image.at[at, place], im_recv.at[at])
            for step in range(1, groups):
                across_copy(at, step).start()
            beside_copy(at, 0).start()

    send_chunks(len(chunks))
    forward_chunks(12)

    @pl.when(section == 0)
    def _():
        for at in range(sections):
            for step in range(1, groups):
                landed(wide, gx_recv.at[at, step])
                beside_copy(at, step).start()

    forward_chunks(len(chunks))
    count_ref[...] = count_finish(2)

    for at in range(1, sections):

        @pl.when(section == at)
        def _():
            image_copy(at).wait_send()

    @pl.when(section == 0)
    def _():
        landed(wide, im_recv.at[0])
        for at in range(sections):
            for step in range(groups):
                landed(wide, gd_recv.at[at, step])
                beside_copy(at, step).wait_send()
                if step > 0:
                    across_copy(at, step).wait_send()
        for item in range(parts):

            @pl.when((group > 0) | (item < AHEAD))
            def _():
                landed(text_first.at[item], tf_recv.at[item])

    for half in range(PAIR):
        here = (section == 0) & (place == half)

        @pl.when(early & jnp.logical_not(here))
        def _():
            text_copy(half).wait_send()

    seg_here.wait()
    for step in range(1, sections):
        landed(seg_all.at[section], seg_recv.at[step])
    for u, (step, source, target) in enumerate(units):
        if u not in direct:
            landed(target, cy_recv.at[u])
    for w in range(len(weights)):
        ref = block_at(w, 0)
        for k in range(sections - 1):

            @pl.when((section >= k) & (section < sections - 1))
            def _():
                landed(ref, up_send.at[w, k])

            @pl.when((section + k <= sections - 1) & (section > 0))
            def _():
                landed(ref, dn_send.at[w, k])

        if weights[w][2] == AFTER:
            for slot in range(sections * replicas):
                if slot % replicas:
                    landed(ref, y_send.at[w, slot])
    for copy in sent:
        copy.wait_send()


def run_vision(patches, vis_gain, vis_bias, loss_mask, segments, shards_of, text, w_query, w_kv, w_out):
    sections = lax.axis_size("section")
    replicas = lax.axis_size("dp")
    parts = lax.axis_size("mp")
    groups = parts // PAIR
    v_qkv, v_out, v_up, v_down, v_proj = shards_of
    total_rows, width = patches.shape
    rows = total_rows // parts
    tokens = rows // 4
    span = v_qkv.shape[2]
    units = (3 * IN_CHUNKS + OUT_BLOCKS - OUT_SHARED) * (groups - 1)
    bf, dma = jnp.bfloat16, pltpu.SemaphoreType.DMA
    vmem = pl.BlockSpec(memory_space=pltpu.VMEM)
    hbm = pl.BlockSpec(memory_space=pl.ANY)
    out_width = v_proj.shape[1]
    slice_width = v_proj.shape[0]
    shape = jax.ShapeDtypeStruct
    image = shape((sections, parts, tokens * parts, out_width), bf)
    levels = parts + replicas + sections
    pair_sem = dma((2, groups))
    ring_sem = dma((5, sections))
    return pl.pallas_call(
        functools.partial(vision_kernel, sections, replicas, parts),
        out_shape=[
            image,
            shape((sections,) + segments.shape[1:], jnp.int32),
            shape((8, loss_mask.shape[1]), jnp.int32),
            shape((parts, text.shape[1] // PAIR, text.shape[2]), bf),
            shape((groups - 1,) + w_query.shape[1:], bf),
            shape((groups - 1,) + w_kv.shape[1:], bf),
            shape((groups - 1,) + w_out.shape[1:], bf),
        ],
        in_specs=[vmem] * 4 + [hbm] * 10,
        out_specs=[hbm] * 2 + [vmem] + [hbm] * 4,
        scratch_shapes=[
            pltpu.VMEM((3, width, span), bf),
            pltpu.VMEM((width, v_out.shape[0]), bf),
            pltpu.VMEM((width, v_up.shape[1]), bf),
            pltpu.VMEM((width, v_down.shape[0]), bf),
            pltpu.VMEM((sections * slice_width, out_width), bf),
            pltpu.VMEM((total_rows, width), bf),
            pltpu.VMEM((3, total_rows, span), bf),
            pltpu.VMEM((total_rows, span), bf),
            pltpu.VMEM((2, total_rows, width), bf),
            pltpu.VMEM((2, groups, rows, width), bf),
            pltpu.VMEM((2, groups, rows, width), bf),
            pltpu.VMEM((2, groups, rows, width), bf),
            pltpu.VMEM((rows, width), bf),
            pltpu.VMEM((total_rows, width), bf),
            pltpu.VMEM((total_rows, v_up.shape[1]), bf),
            pltpu.VMEM((4, tokens, width), bf),
            pltpu.VMEM((replicas, 4, tokens * parts, slice_width), bf),
            pltpu.VMEM((replicas, tokens * parts, out_width), jnp.float32),
            pltpu.VMEM((replicas, tokens * parts, out_width), bf),
            pltpu.VMEM((replicas, tokens * parts, out_width), bf),
            pltpu.VMEM((tokens * parts, out_width), bf),
            pltpu.VMEM((levels, 8, loss_mask.shape[1]), jnp.int32),
            pltpu.VMEM((3, 8, loss_mask.shape[1]), jnp.int32),
            dma((5,)),
            dma((5, sections * replicas)),
            dma((5, sections * replicas)),
            ring_sem,
            ring_sem,
            ring_sem,
            ring_sem,
            pair_sem,
            pair_sem,
            pair_sem,
            pair_sem,
            pair_sem,
            pair_sem,
            pair_sem,
            pair_sem,
            dma((replicas,)),
            dma((replicas,)),
            dma((replicas,)),
            dma((replicas,)),
            dma((1,)),
            dma((sections,)),
            dma((sections, groups)),
            dma((sections, groups)),
            dma((sections, groups)),
            dma((sections, groups)),
            dma((units,)),
            dma((units,)),
            dma((units,)),
            dma((units,)),
            dma((PAIR,)),
            dma((parts,)),
            dma((sections,)),
            dma((sections,)),
            dma((levels,)),
            dma((levels,)),
        ],
        compiler_params=pltpu.CompilerParams(
            has_side_effects=True, vmem_limit_bytes=48 * 1024 * 1024
        ),
    )(
        patches,
        vis_gain,
        vis_bias,
        loss_mask,
        segments,
        v_qkv,
        v_out.T,
        v_up,
        v_down.T,
        v_proj,
        text,
        w_query,
        w_kv,
        w_out,
    )


def decoder_kernel(
    sections,
    parts,
    seqs,
    pick_ref,
    seg_row_ref,
    seg_col_ref,
    gain_ref,
    cos_ref,
    sin_ref,
    image_ref,
    text_ref,
    first_ref,
    *refs,
):
    groups = parts // PAIR
    weight_refs = refs[: len(refs) - 27]
    (
        out_ref,
        w_in,
        w_out,
        arrived,
        normed,
        query,
        keyed,
        valued,
        bias,
        mixed,
        part,
        kept,
        give,
        take,
        done,
        home,
        w_sem,
        text_send,
        text_recv,
        n_send,
        n_recv,
        rs_send,
        rs_recv,
        hop_send,
        hop_recv,
        home_recv,
        turn,
    ) = refs[len(refs) - 27 :]
    section = lax.axis_index("section")
    place = lax.axis_index("mp")
    low = lax.rem(place, PAIR)
    group = place // PAIR
    partner = group * PAIR + (1 - low)
    items, own, width = arrived.shape
    chunk = PAIR * own
    piece = width // PIECES
    kv_width = keyed.shape[1]
    pair_heads = kv_width // HD
    heads = query.shape[0]
    each = heads // pair_heads
    last = sections - 1

    text_group = lax.rem(section, groups)
    text_item = (section // groups) * parts + place

    def text_copy(half):
        return pltpu.make_async_remote_copy(
            src_ref=text_ref.at[0, pl.ds(half * own, own)],
            dst_ref=arrived.at[text_item],
            send_sem=text_send.at[half],
            recv_sem=text_recv.at[text_item],
            device_id={"section": 0, "mp": text_group * PAIR + half},
            device_id_type=MESH,
        )

    @pl.when(section == 0)
    def _():
        for item in range(parts):

            @pl.when((group > 0) | (item < AHEAD))
            def _():
                pltpu.make_async_copy(
                    first_ref.at[item], arrived.at[item], text_recv.at[item]
                ).start()

    later = ((section == 0) & (place >= AHEAD)) | (section >= groups)
    opens = (section // groups == 1) & (place == 0)
    for half in range(PAIR):
        here = (section == 0) & (place == text_group * PAIR + half)

        @pl.when(later & here)
        def _():
            pltpu.make_async_copy(
                text_ref.at[0, pl.ds(half * own, own)],
                arrived.at[text_item],
                text_recv.at[text_item],
            ).start()

        @pl.when(later & (section == 0) & (place < PAIR) & jnp.logical_not(here))
        def _():
            text_copy(half).start()

    in_loads, out_loads = weight_loads(weight_refs, w_in, w_out, groups)
    copies = [
        pltpu.make_async_copy(source, target, w_sem.at[at])
        for at, (source, target) in enumerate(in_loads + out_loads)
    ]
    for copy in copies:
        copy.start()
    keyed[...] = jnp.zeros_like(keyed)
    valued[...] = jnp.zeros_like(valued)
    first_count = len(in_loads)

    @pl.when(later & (section > 0))
    def _():
        @pl.when(jnp.logical_not(opens))
        def _():
            pl.semaphore_wait(turn, 1)

        for half in range(PAIR):
            text_copy(half).start()
        text_copy(0).wait_send()

        @pl.when(place < parts - 1)
        def _():
            pl.semaphore_signal(
                turn, 1, device_id={"mp": lax.rem(place + 1, parts)}, device_id_type=MESH
            )

        @pl.when((place == parts - 1) & (section + groups < sections))
        def _():
            pl.semaphore_signal(
                turn,
                1,
                device_id={"section": lax.rem(section + groups, sections), "mp": 0},
                device_id_type=MESH,
            )

    def one_item(item, carry):
        seq = item // parts
        at = lax.rem(item, parts)
        rows = pl.ds(pl.multiple_of(at * chunk, chunk), chunk)
        own_rows = pl.ds(pl.multiple_of(low * own, own), own)
        other_rows = pl.ds(pl.multiple_of((1 - low) * own, own), own)

        @pl.when((section == 0) & (place >= PAIR) & (item == place - PAIR))
        def _():
            for half in range(PAIR):
                text_copy(half).start()

        @pl.when(section == 0)
        def _():
            pltpu.make_async_copy(arrived.at[item], arrived.at[item], text_recv.at[item]).wait()
            cover = jnp.full((own, 1), pick_ref[item, 2], jnp.int32) > 0
            span = image_ref.shape[-1]
            for p in range(parts):
                cols = slice(p * span, (p + 1) * span)
                arrived[item, :, cols] = jnp.where(
                    cover, image_ref[pick_ref[item, 0], p, pick_ref[item, 1]], arrived[item, :, cols]
                )

        @pl.when(section > 0)
        def _():
            for t in range(PIECES):
                ref = arrived.at[item, :, pl.ds(t * piece, piece)]
                pltpu.make_async_copy(ref, ref, hop_recv.at[item, t]).wait()

        for r in range(0, own, 16):
            wide = arrived[item, r : r + 16, :].astype(jnp.float32)
            power = jnp.mean(wide * wide, axis=-1, keepdims=True)
            to = pl.ds(pl.multiple_of(low * own + r, 16), 16)
            normed[item, to, :] = (wide * lax.rsqrt(power + EPS) * gain_ref[...]).astype(
                jnp.bfloat16
            )
        n_copy = pltpu.make_async_remote_copy(
            src_ref=normed.at[item, own_rows],
            dst_ref=normed.at[item, own_rows],
            send_sem=n_send.at[item],
            recv_sem=n_recv.at[item],
            device_id={"mp": partner},
            device_id_type=MESH,
        )
        n_copy.start()
        allowed = (seg_col_ref[seq, rows, :] == seg_row_ref[seq]) & (
            lax.broadcasted_iota(jnp.int32, bias.shape, 1)
            <= lax.broadcasted_iota(jnp.int32, bias.shape, 0) + at * chunk
        )
        bias[...] = jnp.where(allowed, 0.0, BLOCKED)

        @pl.when(item == 0)
        def _():
            for copy in copies[:first_count]:
                copy.wait()

        n_copy.wait_recv()

        cosine, sinus = cos_ref[rows, :], sin_ref[rows, :]

        def turned(col):
            made = jnp.dot(
                normed[item],
                w_in[:, pl.ds(pl.multiple_of(col, kv_width), kv_width)],
                preferred_element_type=jnp.float32,
            )
            outs = []
            for h in range(pair_heads):
                head = made[:, h * HD : (h + 1) * HD]
                outs.append(
                    (head * cosine + pltpu.roll(head, HD // 2, 1) * sinus).astype(jnp.bfloat16)
                )
            return outs

        def query_tile(tile, c):
            for h, value in enumerate(turned(tile * kv_width)):
                query[tile * pair_heads + h] = value
            return c

        lax.fori_loop(0, heads // pair_heads, query_tile, 0)
        for h, value in enumerate(turned(heads * HD)):
            keyed[rows, h * HD : (h + 1) * HD] = value
        valued[rows, :] = jnp.dot(
            normed[item],
            w_in[:, heads * HD + kv_width :],
            preferred_element_type=jnp.float32,
        ).astype(jnp.bfloat16)

        for h in range(heads):
            kv = slice((h // each) * HD, (h // each + 1) * HD)
            scores = (
                lax.dot_general(
                    query[h],
                    keyed[:, kv],
                    (((1,), (1,)), ((), ())),
                    preferred_element_type=jnp.float32,
                )
                * HD ** (-0.5)
                + bias[...]
            )
            high = jnp.max(scores, axis=-1, keepdims=True)
            grown = jnp.exp(scores - high)
            probs = (grown / jnp.sum(grown, axis=-1, keepdims=True)).astype(jnp.bfloat16)
            mixed[:, h * HD : (h + 1) * HD] = jnp.dot(
                probs, valued[:, kv], preferred_element_type=jnp.float32
            ).astype(jnp.bfloat16)

        @pl.when(item == 0)
        def _():
            for copy in copies[first_count:]:
                copy.wait()

        def give_copy(t):
            return pltpu.make_async_remote_copy(
                src_ref=give.at[item, :, pl.ds(t * piece, piece)],
                dst_ref=take.at[item, :, pl.ds(t * piece, piece)],
                send_sem=rs_send.at[item, t],
                recv_sem=rs_recv.at[item, t],
                device_id={"mp": partner},
                device_id_type=MESH,
            )

        for t in range(PIECES):
            cols = slice(t * piece, (t + 1) * piece)
            part[...] = jnp.dot(mixed[...], w_out[:, cols], preferred_element_type=jnp.float32)
            give[item, :, cols] = part[other_rows, :].astype(jnp.bfloat16)
            give_copy(t).start()
            kept[:, cols] = part[own_rows, :] + arrived[item, :, cols].astype(jnp.float32)

        goal = seq * groups + group
        stays = (section == last) & (goal == last) & (at == place)
        for t in range(PIECES):
            cols = slice(t * piece, (t + 1) * piece)
            give_copy(t).wait_recv()
            done[item, :, cols] = (
                kept[:, cols] + take[item, :, cols].astype(jnp.float32)
            ).astype(jnp.bfloat16)

            @pl.when(section < last)
            def _():
                hop_copy(item, t).start()

            @pl.when((section == last) & jnp.logical_not(stays))
            def _():
                home_copy(item, t).start()

            @pl.when(stays)
            def _():
                home[own_rows, cols] = done[item, :, cols]

        return carry

    def hop_copy(item, t):
        return pltpu.make_async_remote_copy(
            src_ref=done.at[item, :, pl.ds(t * piece, piece)],
            dst_ref=arrived.at[item, :, pl.ds(t * piece, piece)],
            send_sem=hop_send.at[item, t],
            recv_sem=hop_recv.at[item, t],
            device_id={"section": lax.rem(section + 1, sections)},
            device_id_type=MESH,
        )

    def home_copy(item, t):
        return pltpu.make_async_remote_copy(
            src_ref=done.at[item, :, pl.ds(t * piece, piece)],
            dst_ref=home.at[pl.ds(pl.multiple_of(low * own, own), own), pl.ds(t * piece, piece)],
            send_sem=hop_send.at[item, t],
            recv_sem=home_recv.at[low, t],
            device_id={"section": (item // parts) * groups + group, "mp": lax.rem(item, parts)},
            device_id_type=MESH,
        )

    lax.fori_loop(0, items, one_item, 0)

    for half in range(PAIR):
        here = (section == 0) & (place == text_group * PAIR + half)

        @pl.when(later & (section == 0) & jnp.logical_not(here))
        def _():
            text_copy(half).wait_send()

    @pl.when(later & (section > 0))
    def _():
        for half in range(1, PAIR):
            text_copy(half).wait_send()

    def drain(item, carry):
        n_ref = normed.at[item, pl.ds(0, own)]
        pltpu.make_async_copy(n_ref, n_ref, n_send.at[item]).wait()
        goal = (item // parts) * groups + group
        stays = (section == last) & (goal == last) & (lax.rem(item, parts) == place)
        for t in range(PIECES):
            ref = give.at[item, :, pl.ds(t * piece, piece)]
            pltpu.make_async_copy(ref, ref, rs_send.at[item, t]).wait()

            @pl.when(jnp.logical_not(stays))
            def _():
                ref = done.at[item, :, pl.ds(t * piece, piece)]
                pltpu.make_async_copy(ref, ref, hop_send.at[item, t]).wait()

        return carry

    lax.fori_loop(0, items, drain, 0)
    for half in range(PAIR):
        sender = lax.rem(section, groups) * PAIR + half

        @pl.when(jnp.logical_not((section == last) & (place == sender)))
        def _():
            for t in range(PIECES):
                ref = home.at[pl.ds(half * own, own), pl.ds(t * piece, piece)]
                pltpu.make_async_copy(ref, ref, home_recv.at[half, t]).wait()

    out_ref[0] = home[...]


def weight_loads(refs, w_in, w_out, groups):
    query_ref, kv_ref, out_ref = refs[:3]
    query_span, kv_span, out_span = query_ref.shape[2], kv_ref.shape[3], out_ref.shape[1]
    keys_at, values_at = query_span * groups, (query_span + kv_span) * groups
    in_loads = [
        (query_ref.at[0], w_in.at[:, pl.ds(0, query_span)]),
        (kv_ref.at[0, 0], w_in.at[:, pl.ds(keys_at, kv_span)]),
        (kv_ref.at[0, 1], w_in.at[:, pl.ds(values_at, kv_span)]),
    ]
    out_loads = [(out_ref.at[0], w_out.at[pl.ds(0, out_span)])]
    other_q, other_kv, other_o = refs[3:]
    for other in range(1, groups):
        cols = pl.ds(other * query_span, query_span)
        in_loads.append((other_q.at[other - 1], w_in.at[:, cols]))
        for index, at in ((0, keys_at), (1, values_at)):
            cols = pl.ds(at + other * kv_span, kv_span)
            in_loads.append((other_kv.at[other - 1, index], w_in.at[:, cols]))
        out_loads.append((other_o.at[other - 1], w_out.at[pl.ds(other * out_span, out_span)]))
    return in_loads, out_loads


def run_decoder(text, first, image, pick, segs, gain, cosine, sinus, weights, sections, parts):
    seqs, length = segs.shape
    width = text.shape[2]
    chunk = text.shape[1]
    own = chunk // PAIR
    items = seqs * parts
    groups = parts // PAIR
    query_width, kv_width = weights[0].shape[2] * groups, weights[1].shape[3] * groups
    joined = query_width + 2 * kv_width
    loads = 4 * groups
    vmem = pl.BlockSpec(memory_space=pltpu.VMEM)
    hbm = pl.BlockSpec(memory_space=pl.ANY)
    smem = pl.BlockSpec(memory_space=pltpu.SMEM)
    dma = pltpu.SemaphoreType.DMA
    bf = jnp.bfloat16
    return pl.pallas_call(
        functools.partial(decoder_kernel, sections, parts, seqs),
        out_shape=jax.ShapeDtypeStruct(text.shape, text.dtype),
        in_specs=[smem] + [vmem] * 6 + [hbm] * (2 + len(weights)),
        out_specs=vmem,
        scratch_shapes=[
            pltpu.VMEM((width, joined), bf),
            pltpu.VMEM((query_width, width), bf),
            pltpu.VMEM((items, own, width), bf),
            pltpu.VMEM((items, chunk, width), bf),
            pltpu.VMEM((query_width // HD, chunk, HD), bf),
            pltpu.VMEM((length, kv_width), bf),
            pltpu.VMEM((length, kv_width), bf),
            pltpu.VMEM((chunk, length), jnp.float32),
            pltpu.VMEM((chunk, query_width), bf),
            pltpu.VMEM((chunk, width // PIECES), jnp.float32),
            pltpu.VMEM((own, width), jnp.float32),
            pltpu.VMEM((items, own, width), bf),
            pltpu.VMEM((items, own, width), bf),
            pltpu.VMEM((items, own, width), bf),
            pltpu.VMEM((chunk, width), bf),
            dma((loads,)),
            dma((PAIR,)),
            dma((items,)),
            dma((items,)),
            dma((items,)),
            dma((items, PIECES)),
            dma((items, PIECES)),
            dma((items, PIECES)),
            dma((items, PIECES)),
            dma((PAIR, PIECES)),
            pltpu.SemaphoreType.REGULAR,
        ],
        compiler_params=pltpu.CompilerParams(
            has_side_effects=True, vmem_limit_bytes=63 * 1024 * 1024
        ),
        cost_estimate=pl.CostEstimate(
            flops=2 * items * chunk * width * (joined + query_width),
            bytes_accessed=2 * width * (joined + query_width),
            transcendentals=0,
        ),
    )(
        pick,
        segs[:, None, :],
        segs[:, :, None],
        gain,
        cosine,
        sinus,
        image,
        text,
        first,
        *weights,
    )


def shards(
    text,
    patches,
    segments,
    loss_mask,
    tile_batch,
    tile_offset,
    attn_gain,
    w_query,
    w_kv,
    w_out,
    vis_gain,
    vis_bias,
    v_qkv,
    v_out,
    v_up,
    v_down,
    v_proj,
):
    sections = lax.axis_size("section")
    replicas = lax.axis_size("dp")
    parts = lax.axis_size("mp")
    groups = parts // PAIR
    part_at = lax.axis_index("mp")
    low_at = part_at % PAIR
    group_at = part_at // PAIR
    length = segments.shape[2]

    image, seg_all, counts, first, other_q, other_kv, other_o = run_vision(
        patches,
        vis_gain,
        vis_bias,
        loss_mask,
        segments,
        (v_qkv, v_out, v_up, v_down, v_proj),
        text,
        w_query,
        w_kv,
        w_out,
    )
    seqs = sections // groups
    seg_mine = jnp.take(seg_all.reshape(seqs, groups, length), group_at, axis=1)
    scaling = float(sections * replicas * length)
    token_weight = loss_mask.astype(jnp.float32) * scaling / jnp.sum(counts).astype(jnp.float32)
    tiles_here = image.shape[2] // POOL
    blocks = (sections, parts, tiles_here, POOL, image.shape[3])

    batch_all = tile_batch[0]
    offset_all = tile_offset[0]
    items = seqs * parts
    item_ids = jnp.arange(items, dtype=jnp.int32)
    item_batch = (item_ids // parts) * groups + group_at
    chunk = text.shape[1]
    item_place = (item_ids % parts) * chunk + low_at * (chunk // PAIR)
    hit = (batch_all[None, :] == item_batch[:, None]) & (
        offset_all[None, :] == item_place[:, None]
    )
    tile_at = jnp.sum(hit * jnp.arange(batch_all.shape[0], dtype=jnp.int32)[None, :], axis=1)
    pick = jnp.stack(
        [tile_at // tiles_here, tile_at % tiles_here, jnp.any(hit, axis=1).astype(jnp.int32)],
        axis=1,
    ).astype(jnp.int32)

    positions = jnp.arange(length, dtype=jnp.int32)
    freqs = ROPE_BASE ** (-2.0 * jnp.arange(HD // 2, dtype=jnp.float32) / HD)
    angles = positions.astype(jnp.float32)[:, None] * freqs[None, :]
    cosine, sinus = jnp.cos(angles), jnp.sin(angles)
    cos_full = jnp.concatenate([cosine, cosine], axis=1)
    sin_full = jnp.concatenate([-sinus, sinus], axis=1)

    hidden = run_decoder(
        text,
        first,
        image.reshape(blocks),
        pick,
        seg_mine,
        attn_gain,
        cos_full,
        sin_full,
        [w_query, w_kv, w_out, other_q, other_kv, other_o],
        sections,
        parts,
    )
    return (hidden, token_weight)


def solution(mesh):
    in_specs = (
        P("section", ("dp", "mp"), None),
        P(("section", "dp"), None),
        P("section", "dp", None),
        P("section", ("dp", "mp")),
        P("dp", None),
        P("dp", None),
        P("section", None),
        P("section", None, "mp"),
        P("section", None, None, "mp"),
        P("section", "mp", None),
        P(),
        P(),
        P(None, ("section", "dp"), "mp"),
        P("mp", ("section", "dp")),
        P(("section", "dp"), "mp"),
        P("mp", ("section", "dp")),
        P(("section", "dp"), "mp"),
    )
    out_specs = (P("section", ("dp", "mp"), None), P("section", ("dp", "mp")))
    return jax.shard_map(shards, mesh=mesh, in_specs=in_specs, out_specs=out_specs, check_vma=False)
```

```python
import functools

import jax
import jax.numpy as jnp
from jax import lax
from jax.experimental import pallas as pl
from jax.experimental.pallas import tpu as pltpu
from jax.sharding import PartitionSpec as P

HD = 128
VHD = 64
GRID = 16
PATCH = 256
POOL = 64


EPS = 1e-05
ROPE_BASE = 500000.0
BLOCKED = -1e30
PAIR = 2
PIECES = 4
MESH = pl.DeviceIdType.MESH


def layer_norm(values, gain, bias):
    wide = values.astype(jnp.float32)
    center = wide - jnp.mean(wide, axis=-1, keepdims=True)
    spread = jnp.mean(center * center, axis=-1, keepdims=True)
    return (center * lax.rsqrt(spread + EPS) * gain + bias).astype(jnp.bfloat16)


def remote(source, target, send_sem, recv_sem, **device):
    return pltpu.make_async_remote_copy(
        src_ref=source,
        dst_ref=target,
        send_sem=send_sem,
        recv_sem=recv_sem,
        device_id=device,
        device_id_type=MESH,
    )


def landed(ref, sem):
    pltpu.make_async_copy(ref, ref, sem).wait()


def block_rows(ref, start, count):
    rows = pl.ds(pl.multiple_of(start, 16), count)
    return ref.at[:, rows] if len(ref.shape) == 3 else ref.at[rows]


IN_CHUNKS = 8
OUT_BLOCKS = 16
OUT_SHARED = 6
AHEAD = 1
FIRST, AFTER, NEVER = 0, 1, 2


def vision_kernel(
    sections,
    replicas,
    parts,
    patches_ref,
    gain_ref,
    bias_ref,
    loss_ref,
    seg_ref,
    qkv_src,
    out_src,
    up_src,
    down_src,
    proj_src,
    text_ref,
    wq_ref,
    wkv_ref,
    wo_ref,
    image,
    seg_all,
    count_ref,
    text_first,
    other_q,
    other_kv,
    other_o,
    w_qkv,
    w_out,
    w_up,
    w_down,
    w_proj,
    n_one,
    qkv,
    mixed,
    partial,
    pair_in,
    group_out,
    group_in,
    resid,
    n_two,
    inner,
    quads,
    pooled,
    summed,
    far_out,
    far_in,
    wide,
    counts,
    count_src,
    local_sem,
    y_send,
    y_recv,
    up_send,
    up_recv,
    dn_send,
    dn_recv,
    pa_send,
    pa_recv,
    pg_send,
    pg_recv,
    ax_send,
    ax_recv,
    ad_send,
    ad_recv,
    pool_send,
    pool_recv,
    far_send,
    far_recv,
    im_send,
    im_recv,
    gx_send,
    gx_recv,
    gd_send,
    gd_recv,
    cx_send,
    cx_recv,
    cy_send,
    cy_recv,
    tf_send,
    tf_recv,
    seg_send,
    seg_recv,
    cnt_send,
    cnt_recv,
):
    groups = parts // PAIR
    section = lax.axis_index("section")
    replica = lax.axis_index("dp")
    place = lax.axis_index("mp")
    low = lax.rem(place, PAIR)
    group = place // PAIR
    partner = group * PAIR + (1 - low)
    after = lax.rem(section + 1, sections)
    before = lax.rem(section + sections - 1, sections)
    even = lax.rem(replica, 2)
    mate = replica + 1 - 2 * even
    total_rows, width = patches_ref.shape
    rows = total_rows // parts
    own_rows = pl.ds(pl.multiple_of(place * rows, rows), rows)
    sent = []

    def go(copy):
        copy.start()
        sent.append(copy)

    axes = (("mp", place, parts), ("dp", replica, replicas), ("section", section, sections))

    def count_start(level):
        axis, at, size = axes[level]
        slot = sum(axes[i][2] for i in range(level))
        counts[slot + at] = count_src[level]
        for step in range(1, size):
            go(
                remote(
                    count_src.at[level],
                    counts.at[slot + at],
                    cnt_send.at[slot + step],
                    cnt_recv.at[slot + step],
                    **{axis: lax.rem(at + step, size)},
                )
            )

    def count_finish(level):
        size = axes[level][2]
        slot = sum(axes[i][2] for i in range(level))
        for step in range(1, size):
            landed(count_src.at[level], cnt_recv.at[slot + step])
        value = counts[slot]
        for at in range(1, size):
            value = value + counts[slot + at]
        return value

    first_row = lax.broadcasted_iota(jnp.int32, count_ref.shape, 0) == 0
    count_src[0] = jnp.where(first_row, jnp.broadcast_to(loss_ref[...], count_ref.shape), 0)
    count_start(0)

    for step in range(1, sections):
        go(
            remote(
                seg_ref.at[0],
                seg_all.at[section],
                seg_send.at[step],
                seg_recv.at[step],
                section=lax.rem(section + step, sections),
            )
        )
    seg_here = pltpu.make_async_copy(seg_ref.at[0], seg_all.at[section], seg_recv.at[0])
    seg_here.start()

    weights = [
        (qkv_src, w_qkv, AFTER),
        (out_src, w_out, AFTER),
        (up_src, w_up, AFTER),
        (down_src, w_down, AFTER),
        (proj_src, w_proj, NEVER),
    ]

    def block_at(w, block):
        source, buffer, kind = weights[w]
        count = source.shape[-2]
        if kind == FIRST:
            return block_rows(buffer, block * replicas * count, replicas * count)
        if kind == AFTER:
            return block_rows(buffer, (block * replicas + replica) * count, count)
        return block_rows(buffer, block * count, count)

    def up_copy(w, k, source, target):
        return remote(source, target, up_send.at[w, k], up_recv.at[w, k], section=after)

    def down_copy(w, k, source, target):
        return remote(source, target, dn_send.at[w, k], dn_recv.at[w, k], section=before)

    def share(w, block, source):
        if weights[w][2] == AFTER:
            for step in range(1, replicas):
                slot = block * replicas + step
                remote(
                    source,
                    block_at(w, block),
                    y_send.at[w, slot],
                    y_recv.at[w, slot],
                    dp=lax.rem(replica + step, replicas),
                ).start()

    def first_share(w):
        source, buffer, kind = weights[w]
        count = source.shape[-2]
        target = block_rows(buffer, (section * replicas + replica) * count, count)
        pltpu.make_async_copy(source, target, local_sem.at[w]).start()
        for step in range(1, replicas):
            go(
                remote(
                    source,
                    target,
                    y_send.at[w, step],
                    y_recv.at[w, step],
                    dp=lax.rem(replica + step, replicas),
                )
            )

    def own_start(w):
        source, buffer, kind = weights[w]
        target = block_at(w, section)
        if kind == FIRST:
            own = block_rows(buffer, 0, source.shape[-2])
            landed(own, local_sem.at[w])
            for step in range(1, replicas):
                landed(own, y_recv.at[w, step])
            source = target
        else:
            pltpu.make_async_copy(source, target, local_sem.at[w]).start()

        @pl.when(section < sections - 1)
        def _():
            up_copy(w, 0, source, target).start()

        @pl.when(section > 0)
        def _():
            down_copy(w, 0, source, target).start()

        share(w, section, source)

    def pump(w, k):
        @pl.when(section >= k + 1)
        def _():
            block = section - 1 - k
            ref = block_at(w, block)
            landed(ref, up_recv.at[w, k])

            @pl.when(section < sections - 1)
            def _():
                up_copy(w, k + 1, ref, ref).start()

            share(w, block, ref)

        @pl.when(section + k + 1 <= sections - 1)
        def _():
            block = section + 1 + k
            ref = block_at(w, block)
            landed(ref, dn_recv.at[w, k])

            @pl.when(section > 0)
            def _():
                down_copy(w, k + 1, ref, ref).start()

            share(w, block, ref)

    def pump_from(w, k):
        for at in range(k, sections - 1):
            pump(w, at)

    def all_here(w):
        if weights[w][2] != FIRST:
            landed(block_at(w, 0), local_sem.at[w])
        if weights[w][2] == AFTER:
            for slot in range(sections * replicas):
                if slot % replicas:
                    landed(block_at(w, 0), y_recv.at[w, slot])

    units, chunks, direct = [], [], []
    for step in range(1, groups):
        depth = wq_ref.shape[1] // 2 // IN_CHUNKS
        for c in range(IN_CHUNKS):
            at = pl.ds(pl.multiple_of((even * IN_CHUNKS + c) * depth, depth), depth)
            chunks.append([len(units) + i for i in range(3)])
            units.append((step, wq_ref.at[0, at], other_q.at[step - 1, at]))
            units.append((step, wkv_ref.at[0, 0, at], other_kv.at[step - 1, 0, at]))
            units.append((step, wkv_ref.at[0, 1, at], other_kv.at[step - 1, 1, at]))
    for step in range(1, groups):
        depth = wo_ref.shape[1] // OUT_BLOCKS
        for c in range(OUT_BLOCKS - OUT_SHARED):
            block = even * OUT_SHARED + c if c < OUT_SHARED else OUT_SHARED + c
            at = pl.ds(pl.multiple_of(block * depth, depth), depth)
            chunks.append([len(units)])
            if c >= OUT_SHARED:
                direct.append(len(units))
            units.append((step, wo_ref.at[0, at], other_o.at[step - 1, at]))
    progress = {"x": 0, "y": 0}

    def send_chunks(upto):
        while progress["x"] < min(upto, len(chunks)):
            for u in chunks[progress["x"]]:
                step, source, target = units[u]
                to = lax.rem(group + step, groups) * PAIR + low
                go(remote(source, target, cx_send.at[u], cx_recv.at[u], mp=to))
            progress["x"] += 1

    def forward_chunks(upto):
        while progress["y"] < min(upto, len(chunks)):
            for u in chunks[progress["y"]]:
                step, source, target = units[u]
                landed(target, cx_recv.at[u])
                if u in direct:
                    continue
                go(remote(target, target, cy_send.at[u], cy_recv.at[u], dp=mate))
            progress["y"] += 1

    own_start(0)
    own_start(1)
    send_chunks(3)

    def first_norm(r, carry):
        at = pl.ds(pl.multiple_of(r * 32, 32), 32)
        n_one[at, :] = layer_norm(patches_ref[at, :], gain_ref[0:1, :], bias_ref[0:1, :])
        return carry

    lax.fori_loop(0, total_rows // 32, first_norm, 0)
    pump(0, 0)
    own_start(2)
    count_src[1] = count_finish(0)
    count_start(1)
    pump_from(0, 1)
    pump_from(1, 0)
    own_start(3)
    all_here(0)
    span = qkv.shape[2]
    for index in range(3):
        qkv[index] = jnp.dot(
            n_one[...], w_qkv[index], preferred_element_type=jnp.float32
        ).astype(jnp.bfloat16)
    pump(2, 0)
    send_chunks(4)

    def one_tile(tile, carry):
        at = pl.ds(pl.multiple_of(tile * PATCH, PATCH), PATCH)
        for low_col in range(0, span, VHD):
            cols = slice(low_col, low_col + VHD)
            scores = lax.dot_general(
                qkv[0, at, cols],
                qkv[1, at, cols],
                (((1,), (1,)), ((), ())),
                preferred_element_type=jnp.float32,
            ) * VHD ** (-0.5)
            grown = jnp.exp(scores - jnp.max(scores, axis=-1, keepdims=True))
            probs = (grown / jnp.sum(grown, axis=-1, keepdims=True)).astype(jnp.bfloat16)
            mixed[at, cols] = jnp.dot(
                probs, qkv[2, at, cols], preferred_element_type=jnp.float32
            ).astype(jnp.bfloat16)
        return carry

    lax.fori_loop(0, total_rows // PATCH, one_tile, 0)
    pump_from(2, 1)
    pump(3, 0)
    all_here(1)

    def projected(use, left, right):
        tile = 256

        def one(n, carry):
            at = pl.ds(pl.multiple_of(n * tile, tile), tile)
            partial[use, :, at] = lax.dot_general(
                left[...],
                right[at, :],
                (((1,), (1,)), ((), ())),
                preferred_element_type=jnp.float32,
            ).astype(jnp.bfloat16)
            return carry

        lax.fori_loop(0, width // tile, one, 0)

    def block_of(use, other, lane):
        start = (lax.rem(group + other, groups) * PAIR + lane) * rows
        return partial.at[use, pl.ds(pl.multiple_of(start, rows), rows)]

    def scatter(use):
        for other in list(range(1, groups)) + [0]:
            go(
                remote(
                    block_of(use, other, 1 - low),
                    pair_in.at[use, other],
                    pa_send.at[use, other],
                    pa_recv.at[use, other],
                    mp=partner,
                )
            )
        for other in range(1, groups):
            landed(pair_in.at[use, other], pa_recv.at[use, other])
            group_out[use, other - 1] = (
                block_of(use, other, low)[...].astype(jnp.float32)
                + pair_in[use, other].astype(jnp.float32)
            ).astype(jnp.bfloat16)
            go(
                remote(
                    group_out.at[use, other - 1],
                    group_in.at[use, other - 1],
                    pg_send.at[use, other],
                    pg_recv.at[use, other],
                    mp=lax.rem(group + other, groups) * PAIR + low,
                )
            )

    def scattered(use):
        landed(pair_in.at[use, 0], pa_recv.at[use, 0])
        value = block_of(use, 0, low)[...].astype(jnp.float32) + pair_in[use, 0].astype(
            jnp.float32
        )
        for other in range(1, groups):
            landed(group_in.at[use, other - 1], pg_recv.at[use, other])
            value = value + group_in[use, other - 1].astype(jnp.float32)
        return value

    def gather_start(use, view):
        mine = view(place)
        for step in range(1, groups):
            to = lax.rem(group + step, groups) * PAIR + low
            go(remote(mine, mine, ax_send.at[use, step], ax_recv.at[use, step], mp=to))
        go(remote(mine, mine, ad_send.at[use, 0], ad_recv.at[use, 0], mp=partner))

    def gather_finish(use, view):
        for step in range(1, groups):
            ref = view(lax.rem(group + groups - step, groups) * PAIR + low)
            landed(ref, ax_recv.at[use, step])
            go(remote(ref, ref, ad_send.at[use, step], ad_recv.at[use, step], mp=partner))
        for step in range(groups):
            landed(view(place), ad_recv.at[use, step])

    projected(0, mixed, w_out)
    scatter(0)
    send_chunks(5)
    pump(3, 1)
    own_start(4)
    resid[...] = (patches_ref[own_rows, :].astype(jnp.float32) + scattered(0)).astype(jnp.bfloat16)
    n_two[own_rows, :] = layer_norm(resid[...], gain_ref[1:2, :], bias_ref[1:2, :])

    def two_view(p):
        return n_two.at[pl.ds(pl.multiple_of(p * rows, rows), rows)]

    gather_start(0, two_view)
    count_src[2] = count_finish(1)
    count_start(2)
    pump_from(3, 2)
    gather_finish(0, two_view)
    send_chunks(7)
    forward_chunks(2)
    all_here(2)

    def hidden_tile(n, carry):
        at = pl.ds(pl.multiple_of(n * 256, 256), 256)
        made = jnp.dot(n_two[...], w_up[:, at], preferred_element_type=jnp.float32)
        inner[:, at] = (0.5 * made * (1.0 + lax.erf(made * 0.5**0.5))).astype(jnp.bfloat16)
        return carry

    lax.fori_loop(0, inner.shape[1] // 256, hidden_tile, 0)
    pump(4, 0)
    forward_chunks(4)
    all_here(3)
    projected(1, inner, w_down)
    scatter(1)
    send_chunks(10)

    states = (resid[...].astype(jnp.float32) + scattered(1)).astype(jnp.bfloat16)
    tokens = rows // 4
    row_id = lax.broadcasted_iota(jnp.int32, (rows, rows), 0)
    col_id = lax.broadcasted_iota(jnp.int32, (rows, rows), 1)
    spot, token = row_id // tokens, row_id % tokens
    across = GRID // 2
    source_row = (2 * (token // across) + spot // 2) * GRID + 2 * (token % across) + spot % 2
    picker = (source_row == col_id).astype(jnp.bfloat16)
    arranged = jnp.dot(picker, states, preferred_element_type=jnp.float32).astype(jnp.bfloat16)
    for spot_at in range(4):
        quads[spot_at] = arranged[spot_at * tokens : (spot_at + 1) * tokens, :]
    slice_width = pooled.shape[3]
    token_rows = pl.ds(pl.multiple_of(place * tokens, tokens), tokens)

    def slice_cols(at):
        return pl.ds(pl.multiple_of(at * slice_width, slice_width), slice_width)

    for step in range(1, replicas):
        to = lax.rem(replica + step, replicas)
        go(
            remote(
                quads.at[:, :, slice_cols(to)],
                pooled.at[replica, :, token_rows, :],
                pool_send.at[step],
                pool_recv.at[step],
                dp=to,
            )
        )
    pooled[replica, :, token_rows, :] = quads[:, :, slice_cols(replica)]
    for step in range(1, replicas):
        landed(pooled.at[replica, :, token_rows, :], pool_recv.at[step])

    def pool_view(p):
        return pooled.at[:, :, pl.ds(pl.multiple_of(p * tokens, tokens), tokens), :]

    gather_start(1, pool_view)
    pump(4, 1)
    item_rows = text_first.shape[1]

    def text_copy(half):
        return remote(
            text_ref.at[0, pl.ds(half * item_rows, item_rows)],
            text_first.at[place],
            tf_send.at[half],
            tf_recv.at[place],
            section=0,
            mp=section * PAIR + half,
        )

    early = ((section == 0) & (place < AHEAD)) | ((section > 0) & (section < groups))
    for half in range(PAIR):
        here = (section == 0) & (place == half)

        @pl.when(early & here)
        def _():
            pltpu.make_async_copy(
                text_ref.at[0, pl.ds(half * item_rows, item_rows)],
                text_first.at[place],
                tf_recv.at[place],
            ).start()

        @pl.when(early & jnp.logical_not(here))
        def _():
            text_copy(half).start()

    gather_finish(1, pool_view)
    send_chunks(14)
    forward_chunks(7)
    pump_from(4, 2)
    all_here(4)
    all_tokens = pooled.shape[2]

    def image_tile(n, carry):
        at = pl.ds(pl.multiple_of(n * 256, 256), 256)
        value = None
        for spot_at in range(4):
            made = jnp.dot(
                pooled[:, spot_at].reshape(replicas * all_tokens, slice_width),
                w_proj[spot_at * slice_width : (spot_at + 1) * slice_width, at],
                preferred_element_type=jnp.float32,
            )
            value = made if value is None else value + made
        summed[:, :, at] = value.reshape(replicas, all_tokens, 256)
        return carry

    lax.fori_loop(0, summed.shape[2] // 256, image_tile, 0)
    for step in range(1, replicas):
        to = lax.rem(replica + step, replicas)
        far_out[step - 1] = summed[to].astype(jnp.bfloat16)
        go(
            remote(
                far_out.at[step - 1],
                far_in.at[step - 1],
                far_send.at[step],
                far_recv.at[step],
                dp=to,
            )
        )
    forward_chunks(8)
    value = summed[replica]
    for step in range(1, replicas):
        landed(far_in.at[step - 1], far_recv.at[step])
        value = value + far_in[step - 1].astype(jnp.float32)
    wide[...] = value.astype(jnp.bfloat16)

    def image_copy(at):
        return remote(wide, image.at[at, place], im_send.at[0], im_recv.at[at], section=0)

    def across_copy(at, step):
        to = lax.rem(group + step, groups) * PAIR + low
        source = wide if at == 0 else image.at[at, place]
        return remote(
            source, image.at[at, place], gx_send.at[at, step], gx_recv.at[at, step], mp=to
        )

    def beside_copy(at, step):
        from_place = lax.rem(group + groups - step, groups) * PAIR + low
        source = wide if at == 0 and step == 0 else image.at[at, from_place]
        return remote(
            source,
            image.at[at, from_place],
            gd_send.at[at, step],
            gd_recv.at[at, step],
            mp=partner,
        )

    for at in range(1, sections):

        @pl.when(section == at)
        def _():
            image_copy(at).start()

    @pl.when(section == 0)
    def _():
        pltpu.make_async_copy(wide, image.at[0, place], im_recv.at[0]).start()
        for at in range(sections):
            if at > 0:
                landed(image.at[at, place], im_recv.at[at])
            for step in range(1, groups):
                across_copy(at, step).start()
            beside_copy(at, 0).start()

    send_chunks(len(chunks))
    forward_chunks(12)

    @pl.when(section == 0)
    def _():
        for at in range(sections):
            for step in range(1, groups):
                landed(wide, gx_recv.at[at, step])
                beside_copy(at, step).start()

    forward_chunks(len(chunks))
    count_ref[...] = count_finish(2)

    for at in range(1, sections):

        @pl.when(section == at)
        def _():
            image_copy(at).wait_send()

    @pl.when(section == 0)
    def _():
        landed(wide, im_recv.at[0])
        for at in range(sections):
            for step in range(groups):
                landed(wide, gd_recv.at[at, step])
                beside_copy(at, step).wait_send()
                if step > 0:
                    across_copy(at, step).wait_send()
        for item in range(parts):

            @pl.when((group > 0) | (item < AHEAD))
            def _():
                landed(text_first.at[item], tf_recv.at[item])

    for half in range(PAIR):
        here = (section == 0) & (place == half)

        @pl.when(early & jnp.logical_not(here))
        def _():
            text_copy(half).wait_send()

    seg_here.wait()
    for step in range(1, sections):
        landed(seg_all.at[section], seg_recv.at[step])
    for u, (step, source, target) in enumerate(units):
        if u not in direct:
            landed(target, cy_recv.at[u])
    for w in range(len(weights)):
        ref = block_at(w, 0)
        for k in range(sections - 1):

            @pl.when((section >= k) & (section < sections - 1))
            def _():
                landed(ref, up_send.at[w, k])

            @pl.when((section + k <= sections - 1) & (section > 0))
            def _():
                landed(ref, dn_send.at[w, k])

        if weights[w][2] == AFTER:
            for slot in range(sections * replicas):
                if slot % replicas:
                    landed(ref, y_send.at[w, slot])
    for copy in sent:
        copy.wait_send()


def run_vision(patches, vis_gain, vis_bias, loss_mask, segments, shards_of, text, w_query, w_kv, w_out):
    sections = lax.axis_size("section")
    replicas = lax.axis_size("dp")
    parts = lax.axis_size("mp")
    groups = parts // PAIR
    v_qkv, v_out, v_up, v_down, v_proj = shards_of
    total_rows, width = patches.shape
    rows = total_rows // parts
    tokens = rows // 4
    span = v_qkv.shape[2]
    units = (3 * IN_CHUNKS + OUT_BLOCKS - OUT_SHARED) * (groups - 1)
    bf, dma = jnp.bfloat16, pltpu.SemaphoreType.DMA
    vmem = pl.BlockSpec(memory_space=pltpu.VMEM)
    hbm = pl.BlockSpec(memory_space=pl.ANY)
    out_width = v_proj.shape[1]
    slice_width = v_proj.shape[0]
    shape = jax.ShapeDtypeStruct
    image = shape((sections, parts, tokens * parts, out_width), bf)
    levels = parts + replicas + sections
    pair_sem = dma((2, groups))
    ring_sem = dma((5, sections))
    return pl.pallas_call(
        functools.partial(vision_kernel, sections, replicas, parts),
        out_shape=[
            image,
            shape((sections,) + segments.shape[1:], jnp.int32),
            shape((8, loss_mask.shape[1]), jnp.int32),
            shape((parts, text.shape[1] // PAIR, text.shape[2]), bf),
            shape((groups - 1,) + w_query.shape[1:], bf),
            shape((groups - 1,) + w_kv.shape[1:], bf),
            shape((groups - 1,) + w_out.shape[1:], bf),
        ],
        in_specs=[vmem] * 4 + [hbm] * 10,
        out_specs=[hbm] * 2 + [vmem] + [hbm] * 4,
        scratch_shapes=[
            pltpu.VMEM((3, width, span), bf),
            pltpu.VMEM((width, v_out.shape[0]), bf),
            pltpu.VMEM((width, v_up.shape[1]), bf),
            pltpu.VMEM((width, v_down.shape[0]), bf),
            pltpu.VMEM((sections * slice_width, out_width), bf),
            pltpu.VMEM((total_rows, width), bf),
            pltpu.VMEM((3, total_rows, span), bf),
            pltpu.VMEM((total_rows, span), bf),
            pltpu.VMEM((2, total_rows, width), bf),
            pltpu.VMEM((2, groups, rows, width), bf),
            pltpu.VMEM((2, groups, rows, width), bf),
            pltpu.VMEM((2, groups, rows, width), bf),
            pltpu.VMEM((rows, width), bf),
            pltpu.VMEM((total_rows, width), bf),
            pltpu.VMEM((total_rows, v_up.shape[1]), bf),
            pltpu.VMEM((4, tokens, width), bf),
            pltpu.VMEM((replicas, 4, tokens * parts, slice_width), bf),
            pltpu.VMEM((replicas, tokens * parts, out_width), jnp.float32),
            pltpu.VMEM((replicas, tokens * parts, out_width), bf),
            pltpu.VMEM((replicas, tokens * parts, out_width), bf),
            pltpu.VMEM((tokens * parts, out_width), bf),
            pltpu.VMEM((levels, 8, loss_mask.shape[1]), jnp.int32),
            pltpu.VMEM((3, 8, loss_mask.shape[1]), jnp.int32),
            dma((5,)),
            dma((5, sections * replicas)),
            dma((5, sections * replicas)),
            ring_sem,
            ring_sem,
            ring_sem,
            ring_sem,
            pair_sem,
            pair_sem,
            pair_sem,
            pair_sem,
            pair_sem,
            pair_sem,
            pair_sem,
            pair_sem,
            dma((replicas,)),
            dma((replicas,)),
            dma((replicas,)),
            dma((replicas,)),
            dma((1,)),
            dma((sections,)),
            dma((sections, groups)),
            dma((sections, groups)),
            dma((sections, groups)),
            dma((sections, groups)),
            dma((units,)),
            dma((units,)),
            dma((units,)),
            dma((units,)),
            dma((PAIR,)),
            dma((parts,)),
            dma((sections,)),
            dma((sections,)),
            dma((levels,)),
            dma((levels,)),
        ],
        compiler_params=pltpu.CompilerParams(
            has_side_effects=True, vmem_limit_bytes=63 * 1024 * 1024
        ),
    )(
        patches,
        vis_gain,
        vis_bias,
        loss_mask,
        segments,
        v_qkv,
        v_out.T,
        v_up,
        v_down.T,
        v_proj,
        text,
        w_query,
        w_kv,
        w_out,
    )


def decoder_kernel(
    sections,
    parts,
    seqs,
    pick_ref,
    seg_row_ref,
    seg_col_ref,
    gain_ref,
    cos_ref,
    sin_ref,
    image_ref,
    text_ref,
    first_ref,
    *refs,
):
    groups = parts // PAIR
    weight_refs = refs[: len(refs) - 27]
    (
        out_ref,
        w_in,
        w_out,
        arrived,
        normed,
        query,
        keyed,
        valued,
        bias,
        mixed,
        part,
        kept,
        give,
        take,
        done,
        home,
        w_sem,
        text_send,
        text_recv,
        n_send,
        n_recv,
        rs_send,
        rs_recv,
        hop_send,
        hop_recv,
        home_recv,
        turn,
    ) = refs[len(refs) - 27 :]
    section = lax.axis_index("section")
    place = lax.axis_index("mp")
    low = lax.rem(place, PAIR)
    group = place // PAIR
    partner = group * PAIR + (1 - low)
    items, own, width = arrived.shape
    chunk = PAIR * own
    piece = width // PIECES
    kv_width = keyed.shape[1]
    pair_heads = kv_width // HD
    heads = query.shape[0]
    each = heads // pair_heads
    last = sections - 1

    text_group = lax.rem(section, groups)
    text_item = (section // groups) * parts + place

    def text_copy(half):
        return pltpu.make_async_remote_copy(
            src_ref=text_ref.at[0, pl.ds(half * own, own)],
            dst_ref=arrived.at[text_item],
            send_sem=text_send.at[half],
            recv_sem=text_recv.at[text_item],
            device_id={"section": 0, "mp": text_group * PAIR + half},
            device_id_type=MESH,
        )

    @pl.when(section == 0)
    def _():
        for item in range(parts):

            @pl.when((group > 0) | (item < AHEAD))
            def _():
                pltpu.make_async_copy(
                    first_ref.at[item], arrived.at[item], text_recv.at[item]
                ).start()

    later = ((section == 0) & (place >= AHEAD)) | (section >= groups)
    opens = (section // groups == 1) & (place == 0)
    for half in range(PAIR):
        here = (section == 0) & (place == text_group * PAIR + half)

        @pl.when(later & here)
        def _():
            pltpu.make_async_copy(
                text_ref.at[0, pl.ds(half * own, own)],
                arrived.at[text_item],
                text_recv.at[text_item],
            ).start()

        @pl.when(later & (section == 0) & (place < PAIR) & jnp.logical_not(here))
        def _():
            text_copy(half).start()

    in_loads, out_loads = weight_loads(weight_refs, w_in, w_out, groups)
    copies = [
        pltpu.make_async_copy(source, target, w_sem.at[at])
        for at, (source, target) in enumerate(in_loads + out_loads)
    ]
    for copy in copies:
        copy.start()
    keyed[...] = jnp.zeros_like(keyed)
    valued[...] = jnp.zeros_like(valued)
    first_count = len(in_loads)

    @pl.when(later & (section > 0))
    def _():
        @pl.when(jnp.logical_not(opens))
        def _():
            pl.semaphore_wait(turn, 1)

        for half in range(PAIR):
            text_copy(half).start()
        text_copy(0).wait_send()

        @pl.when(place < parts - 1)
        def _():
            pl.semaphore_signal(
                turn, 1, device_id={"mp": lax.rem(place + 1, parts)}, device_id_type=MESH
            )

        @pl.when((place == parts - 1) & (section + groups < sections))
        def _():
            pl.semaphore_signal(
                turn,
                1,
                device_id={"section": lax.rem(section + groups, sections), "mp": 0},
                device_id_type=MESH,
            )

    def one_item(item, carry):
        seq = item // parts
        at = lax.rem(item, parts)
        rows = pl.ds(pl.multiple_of(at * chunk, chunk), chunk)
        own_rows = pl.ds(pl.multiple_of(low * own, own), own)
        other_rows = pl.ds(pl.multiple_of((1 - low) * own, own), own)

        @pl.when((section == 0) & (place >= PAIR) & (item == place - PAIR))
        def _():
            for half in range(PAIR):
                text_copy(half).start()

        @pl.when(section == 0)
        def _():
            pltpu.make_async_copy(arrived.at[item], arrived.at[item], text_recv.at[item]).wait()
            cover = jnp.full((own, 1), pick_ref[item, 2], jnp.int32) > 0
            span = image_ref.shape[-1]
            for p in range(parts):
                cols = slice(p * span, (p + 1) * span)
                arrived[item, :, cols] = jnp.where(
                    cover, image_ref[pick_ref[item, 0], p, pick_ref[item, 1]], arrived[item, :, cols]
                )

        @pl.when(section > 0)
        def _():
            for t in range(PIECES):
                ref = arrived.at[item, :, pl.ds(t * piece, piece)]
                pltpu.make_async_copy(ref, ref, hop_recv.at[item, t]).wait()

        for r in range(0, own, 16):
            wide = arrived[item, r : r + 16, :].astype(jnp.float32)
            power = jnp.mean(wide * wide, axis=-1, keepdims=True)
            to = pl.ds(pl.multiple_of(low * own + r, 16), 16)
            normed[item, to, :] = (wide * lax.rsqrt(power + EPS) * gain_ref[...]).astype(
                jnp.bfloat16
            )
        n_copy = pltpu.make_async_remote_copy(
            src_ref=normed.at[item, own_rows],
            dst_ref=normed.at[item, own_rows],
            send_sem=n_send.at[item],
            recv_sem=n_recv.at[item],
            device_id={"mp": partner},
            device_id_type=MESH,
        )
        n_copy.start()
        allowed = (seg_col_ref[seq, rows, :] == seg_row_ref[seq]) & (
            lax.broadcasted_iota(jnp.int32, bias.shape, 1)
            <= lax.broadcasted_iota(jnp.int32, bias.shape, 0) + at * chunk
        )
        bias[...] = jnp.where(allowed, 0.0, BLOCKED)

        @pl.when(item == 0)
        def _():
            for copy in copies[:first_count]:
                copy.wait()

        n_copy.wait_recv()

        cosine, sinus = cos_ref[rows, :], sin_ref[rows, :]

        def turned(col):
            made = jnp.dot(
                normed[item],
                w_in[:, pl.ds(pl.multiple_of(col, kv_width), kv_width)],
                preferred_element_type=jnp.float32,
            )
            outs = []
            for h in range(pair_heads):
                head = made[:, h * HD : (h + 1) * HD]
                outs.append(
                    (head * cosine + pltpu.roll(head, HD // 2, 1) * sinus).astype(jnp.bfloat16)
                )
            return outs

        def query_tile(tile, c):
            for h, value in enumerate(turned(tile * kv_width)):
                query[tile * pair_heads + h] = value
            return c

        lax.fori_loop(0, heads // pair_heads, query_tile, 0)
        for h, value in enumerate(turned(heads * HD)):
            keyed[rows, h * HD : (h + 1) * HD] = value
        valued[rows, :] = jnp.dot(
            normed[item],
            w_in[:, heads * HD + kv_width :],
            preferred_element_type=jnp.float32,
        ).astype(jnp.bfloat16)

        for h in range(heads):
            kv = slice((h // each) * HD, (h // each + 1) * HD)
            scores = (
                lax.dot_general(
                    query[h],
                    keyed[:, kv],
                    (((1,), (1,)), ((), ())),
                    preferred_element_type=jnp.float32,
                )
                * HD ** (-0.5)
                + bias[...]
            )
            high = jnp.max(scores, axis=-1, keepdims=True)
            grown = jnp.exp(scores - high)
            probs = (grown / jnp.sum(grown, axis=-1, keepdims=True)).astype(jnp.bfloat16)
            mixed[:, h * HD : (h + 1) * HD] = jnp.dot(
                probs, valued[:, kv], preferred_element_type=jnp.float32
            ).astype(jnp.bfloat16)

        @pl.when(item == 0)
        def _():
            for copy in copies[first_count:]:
                copy.wait()

        def give_copy(t):
            return pltpu.make_async_remote_copy(
                src_ref=give.at[item, :, pl.ds(t * piece, piece)],
                dst_ref=take.at[item, :, pl.ds(t * piece, piece)],
                send_sem=rs_send.at[item, t],
                recv_sem=rs_recv.at[item, t],
                device_id={"mp": partner},
                device_id_type=MESH,
            )

        for t in range(PIECES):
            cols = slice(t * piece, (t + 1) * piece)
            part[...] = jnp.dot(mixed[...], w_out[:, cols], preferred_element_type=jnp.float32)
            give[item, :, cols] = part[other_rows, :].astype(jnp.bfloat16)
            give_copy(t).start()
            kept[:, cols] = part[own_rows, :] + arrived[item, :, cols].astype(jnp.float32)

        goal = seq * groups + group
        stays = (section == last) & (goal == last) & (at == place)
        for t in range(PIECES):
            cols = slice(t * piece, (t + 1) * piece)
            give_copy(t).wait_recv()
            done[item, :, cols] = (
                kept[:, cols] + take[item, :, cols].astype(jnp.float32)
            ).astype(jnp.bfloat16)

            @pl.when(section < last)
            def _():
                hop_copy(item, t).start()

            @pl.when((section == last) & jnp.logical_not(stays))
            def _():
                home_copy(item, t).start()

            @pl.when(stays)
            def _():
                home[own_rows, cols] = done[item, :, cols]

        return carry

    def hop_copy(item, t):
        return pltpu.make_async_remote_copy(
            src_ref=done.at[item, :, pl.ds(t * piece, piece)],
            dst_ref=arrived.at[item, :, pl.ds(t * piece, piece)],
            send_sem=hop_send.at[item, t],
            recv_sem=hop_recv.at[item, t],
            device_id={"section": lax.rem(section + 1, sections)},
            device_id_type=MESH,
        )

    def home_copy(item, t):
        return pltpu.make_async_remote_copy(
            src_ref=done.at[item, :, pl.ds(t * piece, piece)],
            dst_ref=home.at[pl.ds(pl.multiple_of(low * own, own), own), pl.ds(t * piece, piece)],
            send_sem=hop_send.at[item, t],
            recv_sem=home_recv.at[low, t],
            device_id={"section": (item // parts) * groups + group, "mp": lax.rem(item, parts)},
            device_id_type=MESH,
        )

    lax.fori_loop(0, items, one_item, 0)

    for half in range(PAIR):
        here = (section == 0) & (place == text_group * PAIR + half)

        @pl.when(later & (section == 0) & jnp.logical_not(here))
        def _():
            text_copy(half).wait_send()

    @pl.when(later & (section > 0))
    def _():
        for half in range(1, PAIR):
            text_copy(half).wait_send()

    def drain(item, carry):
        n_ref = normed.at[item, pl.ds(0, own)]
        pltpu.make_async_copy(n_ref, n_ref, n_send.at[item]).wait()
        goal = (item // parts) * groups + group
        stays = (section == last) & (goal == last) & (lax.rem(item, parts) == place)
        for t in range(PIECES):
            ref = give.at[item, :, pl.ds(t * piece, piece)]
            pltpu.make_async_copy(ref, ref, rs_send.at[item, t]).wait()

            @pl.when(jnp.logical_not(stays))
            def _():
                ref = done.at[item, :, pl.ds(t * piece, piece)]
                pltpu.make_async_copy(ref, ref, hop_send.at[item, t]).wait()

        return carry

    lax.fori_loop(0, items, drain, 0)
    for half in range(PAIR):
        sender = lax.rem(section, groups) * PAIR + half

        @pl.when(jnp.logical_not((section == last) & (place == sender)))
        def _():
            for t in range(PIECES):
                ref = home.at[pl.ds(half * own, own), pl.ds(t * piece, piece)]
                pltpu.make_async_copy(ref, ref, home_recv.at[half, t]).wait()

    out_ref[0] = home[...]


def weight_loads(refs, w_in, w_out, groups):
    query_ref, kv_ref, out_ref = refs[:3]
    query_span, kv_span, out_span = query_ref.shape[2], kv_ref.shape[3], out_ref.shape[1]
    keys_at, values_at = query_span * groups, (query_span + kv_span) * groups
    in_loads = [
        (query_ref.at[0], w_in.at[:, pl.ds(0, query_span)]),
        (kv_ref.at[0, 0], w_in.at[:, pl.ds(keys_at, kv_span)]),
        (kv_ref.at[0, 1], w_in.at[:, pl.ds(values_at, kv_span)]),
    ]
    out_loads = [(out_ref.at[0], w_out.at[pl.ds(0, out_span)])]
    other_q, other_kv, other_o = refs[3:]
    for other in range(1, groups):
        cols = pl.ds(other * query_span, query_span)
        in_loads.append((other_q.at[other - 1], w_in.at[:, cols]))
        for index, at in ((0, keys_at), (1, values_at)):
            cols = pl.ds(at + other * kv_span, kv_span)
            in_loads.append((other_kv.at[other - 1, index], w_in.at[:, cols]))
        out_loads.append((other_o.at[other - 1], w_out.at[pl.ds(other * out_span, out_span)]))
    return in_loads, out_loads


def run_decoder(text, first, image, pick, segs, gain, cosine, sinus, weights, sections, parts):
    seqs, length = segs.shape
    width = text.shape[2]
    chunk = text.shape[1]
    own = chunk // PAIR
    items = seqs * parts
    groups = parts // PAIR
    query_width, kv_width = weights[0].shape[2] * groups, weights[1].shape[3] * groups
    joined = query_width + 2 * kv_width
    loads = 4 * groups
    vmem = pl.BlockSpec(memory_space=pltpu.VMEM)
    hbm = pl.BlockSpec(memory_space=pl.ANY)
    smem = pl.BlockSpec(memory_space=pltpu.SMEM)
    dma = pltpu.SemaphoreType.DMA
    bf = jnp.bfloat16
    return pl.pallas_call(
        functools.partial(decoder_kernel, sections, parts, seqs),
        out_shape=jax.ShapeDtypeStruct(text.shape, text.dtype),
        in_specs=[smem] + [vmem] * 6 + [hbm] * (2 + len(weights)),
        out_specs=vmem,
        scratch_shapes=[
            pltpu.VMEM((width, joined), bf),
            pltpu.VMEM((query_width, width), bf),
            pltpu.VMEM((items, own, width), bf),
            pltpu.VMEM((items, chunk, width), bf),
            pltpu.VMEM((query_width // HD, chunk, HD), bf),
            pltpu.VMEM((length, kv_width), bf),
            pltpu.VMEM((length, kv_width), bf),
            pltpu.VMEM((chunk, length), jnp.float32),
            pltpu.VMEM((chunk, query_width), bf),
            pltpu.VMEM((chunk, width // PIECES), jnp.float32),
            pltpu.VMEM((own, width), jnp.float32),
            pltpu.VMEM((items, own, width), bf),
            pltpu.VMEM((items, own, width), bf),
            pltpu.VMEM((items, own, width), bf),
            pltpu.VMEM((chunk, width), bf),
            dma((loads,)),
            dma((PAIR,)),
            dma((items,)),
            dma((items,)),
            dma((items,)),
            dma((items, PIECES)),
            dma((items, PIECES)),
            dma((items, PIECES)),
            dma((items, PIECES)),
            dma((PAIR, PIECES)),
            pltpu.SemaphoreType.REGULAR,
        ],
        compiler_params=pltpu.CompilerParams(
            has_side_effects=True, vmem_limit_bytes=63 * 1024 * 1024
        ),
        cost_estimate=pl.CostEstimate(
            flops=2 * items * chunk * width * (joined + query_width),
            bytes_accessed=2 * width * (joined + query_width),
            transcendentals=0,
        ),
    )(
        pick,
        segs[:, None, :],
        segs[:, :, None],
        gain,
        cosine,
        sinus,
        image,
        text,
        first,
        *weights,
    )


def shards(
    text,
    patches,
    segments,
    loss_mask,
    tile_batch,
    tile_offset,
    attn_gain,
    w_query,
    w_kv,
    w_out,
    vis_gain,
    vis_bias,
    v_qkv,
    v_out,
    v_up,
    v_down,
    v_proj,
):
    sections = lax.axis_size("section")
    replicas = lax.axis_size("dp")
    parts = lax.axis_size("mp")
    groups = parts // PAIR
    part_at = lax.axis_index("mp")
    low_at = part_at % PAIR
    group_at = part_at // PAIR
    length = segments.shape[2]

    image, seg_all, counts, first, other_q, other_kv, other_o = run_vision(
        patches,
        vis_gain,
        vis_bias,
        loss_mask,
        segments,
        (v_qkv, v_out, v_up, v_down, v_proj),
        text,
        w_query,
        w_kv,
        w_out,
    )
    seqs = sections // groups
    seg_mine = jnp.take(seg_all.reshape(seqs, groups, length), group_at, axis=1)
    scaling = float(sections * replicas * length)
    token_weight = loss_mask.astype(jnp.float32) * scaling / jnp.sum(counts).astype(jnp.float32)
    tiles_here = image.shape[2] // POOL
    blocks = (sections, parts, tiles_here, POOL, image.shape[3])

    batch_all = tile_batch[0]
    offset_all = tile_offset[0]
    items = seqs * parts
    item_ids = jnp.arange(items, dtype=jnp.int32)
    item_batch = (item_ids // parts) * groups + group_at
    chunk = text.shape[1]
    item_place = (item_ids % parts) * chunk + low_at * (chunk // PAIR)
    hit = (batch_all[None, :] == item_batch[:, None]) & (
        offset_all[None, :] == item_place[:, None]
    )
    tile_at = jnp.sum(hit * jnp.arange(batch_all.shape[0], dtype=jnp.int32)[None, :], axis=1)
    pick = jnp.stack(
        [tile_at // tiles_here, tile_at % tiles_here, jnp.any(hit, axis=1).astype(jnp.int32)],
        axis=1,
    ).astype(jnp.int32)

    positions = jnp.arange(length, dtype=jnp.int32)
    freqs = ROPE_BASE ** (-2.0 * jnp.arange(HD // 2, dtype=jnp.float32) / HD)
    angles = positions.astype(jnp.float32)[:, None] * freqs[None, :]
    cosine, sinus = jnp.cos(angles), jnp.sin(angles)
    cos_full = jnp.concatenate([cosine, cosine], axis=1)
    sin_full = jnp.concatenate([-sinus, sinus], axis=1)

    hidden = run_decoder(
        text,
        first,
        image.reshape(blocks),
        pick,
        seg_mine,
        attn_gain,
        cos_full,
        sin_full,
        [w_query, w_kv, w_out, other_q, other_kv, other_o],
        sections,
        parts,
    )
    return (hidden, token_weight)


def solution(mesh):
    in_specs = (
        P("section", ("dp", "mp"), None),
        P(("section", "dp"), None),
        P("section", "dp", None),
        P("section", ("dp", "mp")),
        P("dp", None),
        P("dp", None),
        P("section", None),
        P("section", None, "mp"),
        P("section", None, None, "mp"),
        P("section", "mp", None),
        P(),
        P(),
        P(None, ("section", "dp"), "mp"),
        P("mp", ("section", "dp")),
        P(("section", "dp"), "mp"),
        P("mp", ("section", "dp")),
        P(("section", "dp"), "mp"),
    )
    out_specs = (P("section", ("dp", "mp"), None), P("section", ("dp", "mp")))
    return jax.shard_map(shards, mesh=mesh, in_specs=in_specs, out_specs=out_specs, check_vma=False)
```
